128 devices in a mesh: seq: 32 (over z, y, core), head: 4 (over x).
Axes of the slice: x: 4, y: 4, z: 4, core: 2. Of those that a mesh axis runs over, the one named last changes fastest.
Arguments:
- queries: bfloat16 [2048, 32, 128], P('seq', 'head'), may hold values from -256 to 256
- keys: bfloat16 [65536, 16, 128], P('seq', 'head'), may hold values from -5 to 5
- values: bfloat16 [65536, 16, 128], P('seq', 'head'), may hold values from -6 to 6
- kv_len: int32 [32], P('seq'), may hold values from 1024 to 2048, as said below
- causal_offset: int32 [1], replicated, may hold values from 61440 to 63488
- out_weight: bfloat16 [4096, 4608], P('head'), may hold values from -0.09375 to 0.09375
Outputs:
- attn_out: float32 [2048, 4608], P('seq', 'head')
The draws below stay inside these ranges and needn't reach their ends.
Inputs may be any that keep to these rules, and one draw needn't show every extreme that they name: `kv_len`: every shard is at least half full and some shard is completely full.
All inputs are finite; a program needn't handle non-finite values.
Results may differ from the reference program's by a relative error of at most 0.006.
Values may be sent and summed in bfloat16 or wider, within the bound.
A program may use at most 192 MiB of HBM per device.

```python
import jax
import jax.numpy as jnp
from jax import lax

D = 4608
QH = 32
KVH = 16
HD = 128
Q_ROWS = 2048
KV_DEV = 2048
SEQ_SHARDS = 32
KV_TOTAL = 65536


def shard_keys(key, shard_idx):
    return jnp.clip(jax.random.normal(jax.random.fold_in(key, shard_idx), (KV_DEV, KVH, HD), jnp.float32), -5.0, 5.0)


def draw_keys(key, part):
    base_key = jax.random.fold_in(key, 7)
    blocks = jax.vmap(lambda shard_idx: shard_keys(base_key, shard_idx))(jnp.arange(SEQ_SHARDS, dtype=jnp.int32))
    return blocks.reshape(SEQ_SHARDS * KV_DEV, KVH, HD).astype(jnp.bfloat16)


def draw_queries(key, part):
    base = jnp.clip(3.0 * jax.random.normal(jax.random.fold_in(key, 11), (Q_ROWS, QH, HD), jnp.float32), -15.0, 15.0)
    return base.astype(jnp.bfloat16)


def draw_kv_len(key, part):
    lengths = jax.random.randint(jax.random.fold_in(key, 21), (SEQ_SHARDS,), KV_DEV // 2, KV_DEV + 1)
    full_idx = jax.random.randint(jax.random.fold_in(key, 22), (), 0, SEQ_SHARDS)
    return lengths.at[full_idx].set(KV_DEV).astype(jnp.int32)


def block_levels(rng, extent, cuts, low, top_value):
    level, own = 1.0, jax.random.fold_in(rng, 6)
    for position, shards_of in cuts:
        heights = jnp.exp(jax.random.uniform(jax.random.fold_in(own, position), (shards_of,), jnp.float32, low / len(cuts), top_value / len(cuts)))
        level = level * jnp.repeat(heights, extent[position] // shards_of).reshape([-1 if axis == position else 1 for axis in range(len(extent))])
    return level


def gaussian(own_key, shape, spread, most, shards=(), kind=jnp.bfloat16):
    loudness = block_levels(own_key, shape, shards, -0.22, 0.18) if shards else 1.0
    result = jax.random.normal(own_key, shape, jnp.float32) * spread * loudness
    return jnp.minimum(jnp.maximum(result, -most), most).astype(kind)


def setup_inputs(seed: int = 0) -> dict:
    arg_keys = jax.random.split(jax.random.key(seed), 7)
    queries = draw_queries(jax.random.fold_in(arg_keys[6], 71), 0)
    keys = draw_keys(jax.random.fold_in(arg_keys[6], 71), 0)
    values = gaussian(arg_keys[2], (KV_TOTAL, KVH, HD), 1.0, 6.0, ((0, 32), (1, 4)))
    kv_len = draw_kv_len(jax.random.fold_in(arg_keys[6], 71), 0)
    causal_offset = jax.random.randint(arg_keys[4], (1,), KV_TOTAL - Q_ROWS - KV_DEV, KV_TOTAL - Q_ROWS + 1).astype(jnp.int32)
    out_weight = gaussian(arg_keys[5], (QH * HD, D), (QH * HD) ** -0.5, 0.09375, ((0, 4),))
    return dict(queries=queries, keys=keys, values=values, kv_len=kv_len, causal_offset=causal_offset, out_weight=out_weight)


score_scale = 1.0 / 12.0
floor_value = -1.0e30


def group_attention(query_pair, key_group, value_group, kv_len, pair_pos):
    def block_scores(shard_idx):
        start = (shard_idx * KV_DEV).astype(jnp.int32)
        key_block = lax.dynamic_slice_in_dim(key_group, start, KV_DEV, 0)
        scores = jnp.dot(query_pair, key_block.T, preferred_element_type=jnp.float32) * score_scale
        slot_idx = jnp.arange(KV_DEV, dtype=jnp.int32)
        key_pos = start + slot_idx
        limit = lax.dynamic_index_in_dim(kv_len, shard_idx, 0, keepdims=False)
        valid = (slot_idx < limit)[None, :] & (key_pos[None, :] <= pair_pos[:, None])
        return scores, valid, start

    def max_step(running, shard_idx):
        scores, valid, start = block_scores(shard_idx)
        return jnp.maximum(running, jnp.max(jnp.where(valid, scores, floor_value), axis=1)), None

    shard_ids = jnp.arange(SEQ_SHARDS, dtype=jnp.int32)
    row_count = query_pair.shape[0]
    row_max, _ = lax.scan(max_step, jnp.full((row_count,), floor_value, jnp.float32), shard_ids)

    def sum_step(carry, shard_idx):
        numer, denom = carry
        scores, valid, start = block_scores(shard_idx)
        weights = jnp.where(valid, jnp.exp(scores - row_max[:, None]), 0.0)
        value_block = lax.dynamic_slice_in_dim(value_group, start, KV_DEV, 0)
        numer = numer + jnp.dot(weights.astype(jnp.bfloat16), value_block, preferred_element_type=jnp.float32)
        denom = denom + jnp.sum(weights, axis=1)
        return (numer, denom), None

    init = (jnp.zeros((row_count, HD), jnp.float32), jnp.zeros((row_count,), jnp.float32))
    (numer, denom), _ = lax.scan(sum_step, init, shard_ids)
    return (numer / denom[:, None]).astype(jnp.bfloat16)


def reference(queries, keys, values, kv_len, causal_offset, out_weight):
    query_pos = causal_offset[0] + jnp.arange(Q_ROWS, dtype=jnp.int32)
    pair_pos = jnp.repeat(query_pos, 2)

    def per_group(group_idx):
        query_pair = lax.dynamic_slice_in_dim(queries, (group_idx * 2).astype(jnp.int32), 2, 1).reshape(Q_ROWS * 2, HD)
        key_group = lax.dynamic_index_in_dim(keys, group_idx, 1, keepdims=False)
        value_group = lax.dynamic_index_in_dim(values, group_idx, 1, keepdims=False)
        return group_attention(query_pair, key_group, value_group, kv_len, pair_pos)

    attended = lax.map(per_group, jnp.arange(KVH, dtype=jnp.int32))
    attended = attended.reshape(KVH, Q_ROWS, 2, HD).transpose(1, 0, 2, 3).reshape(Q_ROWS, QH * HD)
    return jnp.dot(attended, out_weight, preferred_element_type=jnp.float32)
```

```python
import functools
import math

import jax
import jax.numpy as jnp
from jax import lax
from jax.experimental import pallas as pl
from jax.experimental.pallas import tpu as pltpu
from jax.sharding import PartitionSpec as P

bf16 = jnp.bfloat16
f32 = jnp.float32
MESH = pl.DeviceIdType.MESH
score_scale = math.log2(math.e) / 12.0
masked_score = -1e30
HD = 128
CHIPS = 16
ROWS = 64
SLOTS = 2048
VROWS = 144
CH = 256
NCH = 2 * SLOTS // CH
VMEM_LIMIT = 60 * 2**20


def place():
    seq = lax.axis_index("seq")
    head = lax.axis_index("head")
    chip = seq // 2
    return seq, head, chip // 4, chip % 4, seq % 2


def dev(z, y, core, head):
    return ((z * 4 + y) * 2 + core, head)


def enter(peers):
    barrier = pltpu.get_barrier_semaphore()
    for peer in peers:
        pl.semaphore_signal(barrier, inc=1, device_id=peer, device_id_type=MESH)
    pl.semaphore_wait(barrier, len(peers))


def remote(src, dst, send_sem, recv_sem, device):
    return pltpu.make_async_remote_copy(
        src_ref=src,
        dst_ref=dst,
        send_sem=send_sem,
        recv_sem=recv_sem,
        device_id=device,
        device_id_type=MESH,
    )


def gather_kernel(
    len_ref, q_ref, k_ref, v_ref, qg, kg, vg,
    wide, qs, ks, vs, local_sem, psend, precv, ysend, yrecv, zsend, zrecv, fsend, frecv,
):
    seq, head, z, y, c = place()
    p = 1 - c
    partner = dev(z, y, p, head)
    peers = [partner]
    for d in (1, 2, 3):
        for tc in (0, 1):
            peers.append(dev(z, (y + d) % 4, tc, head))
            peers.append(dev((z + d) % 4, y, tc, head))

    wide[0:512, :] = q_ref[...].astype(f32)
    for h in range(8):
        qs[h] = wide[pl.ds(h, ROWS, stride=8), :].astype(bf16)
    enter(peers)

    first = []
    own = (z * 4 + y) * 2 + c
    copy = remote(qs.at[pl.ds(4 * p, 4)], qg.at[z, y, c], psend.at[0], precv.at[0], partner)
    copy.start()
    first.append(copy)
    for d in (1, 2, 3):
        for tc in (0, 1):
            copy = remote(
                qs.at[pl.ds(4 * tc, 2)], qg.at[z, y, c, pl.ds(0, 2)],
                ysend.at[d - 1, tc], yrecv.at[d - 1, c], dev(z, (y + d) % 4, tc, head),
            )
            copy.start()
            first.append(copy)
            copy = remote(
                qs.at[pl.ds(4 * tc + 2, 2)], qg.at[z, y, c, pl.ds(2, 2)],
                zsend.at[d - 1, tc], zrecv.at[d - 1, c], dev((z + d) % 4, y, tc, head),
            )
            copy.start()
            first.append(copy)
    mine_q = pltpu.make_async_copy(qs.at[pl.ds(4 * c, 4)], qg.at[z, y, c], local_sem.at[0])
    mine_q.start()

    length = len_ref[0]
    rows = 256
    k0 = k_ref[0:8, :].astype(f32)

    def relayout(b, _):
        slot = lax.broadcasted_iota(jnp.int32, (rows, HD), 0) + b * rows
        filled = slot < length
        wide[...] = k_ref[pl.ds(pl.multiple_of(b * rows * 4, rows * 4), rows * 4), :].astype(f32)
        for h in range(4):
            part = wide[pl.ds(h, rows, stride=4), :]
            part = jnp.where(filled, part, k0[h : h + 1, :])
            ks[h, pl.ds(pl.multiple_of(b * rows, rows), rows), :] = part.astype(bf16)
        wide[...] = v_ref[pl.ds(pl.multiple_of(b * rows * 4, rows * 4), rows * 4), :].astype(f32)
        col = lax.broadcasted_iota(jnp.int32, (16, rows), 1) + b * rows
        row = lax.broadcasted_iota(jnp.int32, (16, rows), 0)
        ones = jnp.where((col < length) & (row == 0), 1.0, 0.0).astype(bf16)
        for h in range(4):
            part = wide[pl.ds(h, rows, stride=4), :]
            part = jnp.where(filled, part, 0.0)
            cols = pl.ds(pl.multiple_of(b * rows, rows), rows)
            vs[h, 0:HD, cols] = part.T.astype(bf16)
            vs[h, HD:VROWS, cols] = ones
        return 0

    lax.fori_loop(0, SLOTS // rows, relayout, 0)
    send_k = remote(ks.at[pl.ds(2 * p, 2)], kg.at[c], psend.at[1], precv.at[1], partner)
    send_v = remote(vs.at[pl.ds(2 * p, 2)], vg.at[c], psend.at[2], precv.at[2], partner)
    send_k.start()
    send_v.start()
    mine_k = pltpu.make_async_copy(ks.at[pl.ds(2 * c, 2)], kg.at[c], local_sem.at[1])
    mine_v = pltpu.make_async_copy(vs.at[pl.ds(2 * c, 2)], vg.at[c], local_sem.at[2])
    mine_k.start()
    mine_v.start()

    mine_q.wait()
    for copy in first:
        copy.wait_send()
    first[0].wait_recv()
    for d in (1, 2, 3):
        for sc in (0, 1):
            remote(
                qs.at[pl.ds(0, 2)], qg.at[z, (y + 4 - d) % 4, sc, pl.ds(0, 2)],
                ysend.at[d - 1, sc], yrecv.at[d - 1, sc], partner,
            ).wait_recv()
            remote(
                qs.at[pl.ds(0, 2)], qg.at[(z + 4 - d) % 4, y, sc, pl.ds(2, 2)],
                zsend.at[d - 1, sc], zrecv.at[d - 1, sc], partner,
            ).wait_recv()

    second = []
    for d in (1, 2, 3):
        src = qg.at[z, :, :, pl.ds(0, 2)]
        copy = remote(src, src, fsend.at[0, d - 1], frecv.at[0, d - 1], dev((z + d) % 4, y, c, head))
        copy.start()
        second.append(copy)
        src = qg.at[:, y, :, pl.ds(2, 2)]
        copy = remote(src, src, fsend.at[1, d - 1], frecv.at[1, d - 1], dev(z, (y + d) % 4, c, head))
        copy.start()
        second.append(copy)
    for copy in second:
        copy.wait_send()
    for d in (1, 2, 3):
        src = qg.at[(z + 4 - d) % 4, :, :, pl.ds(0, 2)]
        remote(src, src, fsend.at[0, d - 1], frecv.at[0, d - 1], partner).wait_recv()
        src = qg.at[:, (y + 4 - d) % 4, :, pl.ds(2, 2)]
        remote(src, src, fsend.at[1, d - 1], frecv.at[1, d - 1], partner).wait_recv()
    send_k.wait()
    send_v.wait()
    mine_k.wait()
    mine_v.wait()


def gather(length, q, k, v):
    dma = pltpu.SemaphoreType.DMA
    vmem = pl.BlockSpec(memory_space=pltpu.VMEM)
    hbm = pl.BlockSpec(memory_space=pl.ANY)
    return pl.pallas_call(
        gather_kernel,
        out_shape=(
            jax.ShapeDtypeStruct((4, 4, 2, 4, ROWS, HD), bf16),
            jax.ShapeDtypeStruct((2, 2, SLOTS, HD), bf16),
            jax.ShapeDtypeStruct((2, 2, VROWS, SLOTS), bf16),
        ),
        in_specs=[pl.BlockSpec(memory_space=pltpu.SMEM), vmem, vmem, vmem],
        out_specs=(hbm, hbm, hbm),
        scratch_shapes=[
            pltpu.VMEM((1024, HD), f32),
            pltpu.VMEM((8, ROWS, HD), bf16),
            pltpu.VMEM((4, SLOTS, HD), bf16),
            pltpu.VMEM((4, VROWS, SLOTS), bf16),
            dma((3,)),
            dma((3,)),
            dma((3,)),
            dma((3, 2)),
            dma((3, 2)),
            dma((3, 2)),
            dma((3, 2)),
            dma((2, 3)),
            dma((2, 3)),
        ],
        compiler_params=pltpu.CompilerParams(
            collective_id=0, has_side_effects=True, vmem_limit_bytes=VMEM_LIMIT
        ),
        name="gather",
    )(length, q, k, v)


def attention_kernel(off_ref, q_ref, k_ref, vt_ref, o_ref, m_ref, s0, s1):
    seq = lax.axis_index("seq")
    last_chip = seq // 2 == CHIPS - 1
    first_key = (SLOTS * 2) * (CHIPS - 1)
    offset = off_ref[0] - first_key

    def queries_of(tile):
        chip, group = tile // 2, tile % 2
        parts = [q_ref[chip // 4, chip % 4, c, group * 2 + h] for h in (0, 1) for c in (0, 1)]
        q = jnp.concatenate(parts, axis=0).astype(f32) * score_scale
        high = q.astype(bf16)
        low = (q - high.astype(f32)).astype(bf16)
        return jnp.concatenate([high, low], axis=1)

    def tiles(tn, sn, tc, sc, m_now, causal):
        m = jnp.full((8, 256), masked_score, f32)
        if tn is not None:
            qq = queries_of(tn)
            if causal:
                lane = lax.broadcasted_iota(jnp.int32, (8, 256), 1) % HD
                limit = offset + (tn // 2) * HD + lane - lax.broadcasted_iota(jnp.int32, (8, 256), 0)
        acc = jnp.zeros((VROWS, 256), f32)
        for c in range(NCH):
            shard, start = c // 8, (c % 8) * CH
            if tn is not None:
                k = k_ref[shard, tn % 2, pl.ds(start, CH), :]
                kk = jnp.concatenate([k, k], axis=1)
                s = lax.dot_general(kk, qq, (((1,), (1,)), ((), ())), preferred_element_type=f32)
                s = s.reshape(CH // 8, 8, 256)
                if causal:
                    s = jnp.stack(
                        [
                            jnp.where(limit >= c * CH + 8 * i, s[i], masked_score)
                            for i in range(CH // 8)
                        ]
                    )
                sn[pl.ds(c * CH, CH), :] = s.reshape(CH, 256)
                m = jnp.maximum(m, jnp.max(s, axis=0))
            if tc is not None:
                s = sc[pl.ds(c * CH, CH), :].reshape(CH // 8, 8, 256)
                prob = jnp.exp2(s - m_now[None]).reshape(CH, 256).astype(bf16)
                vt = vt_ref[shard, tc % 2, :, pl.ds(start, CH)]
                acc = acc + jnp.dot(vt, prob, preferred_element_type=f32)
        if tc is not None:
            chip, group = tc // 2, tc % 2
            o_ref[chip // 4, chip % 4, group] = acc[:HD].astype(bf16)
            m_ref[chip // 4, chip % 4, group, 0:1, :] = m_now[0:1]
            m_ref[chip // 4, chip % 4, group, 1:2, :] = acc[HD : HD + 1]
        if tn is not None:
            return jnp.broadcast_to(jnp.max(m, axis=0, keepdims=True), (8, 256))

    def run(causal):
        m = tiles(0, s0, None, None, None, causal)

        def body(u, m):
            m = tiles(2 * u + 1, s1, 2 * u, s0, m, causal)
            return tiles(jnp.minimum(2 * u + 2, 31), s0, 2 * u + 1, s1, m, causal)

        lax.fori_loop(0, CHIPS, body, m)

    @pl.when(jnp.logical_not(last_chip))
    def _():
        run(False)

    @pl.when(last_chip)
    def _():
        run(True)


def attention(offset, q, k, vt):
    vmem = pl.BlockSpec(memory_space=pltpu.VMEM)
    return pl.pallas_call(
        attention_kernel,
        out_shape=(
            jax.ShapeDtypeStruct((4, 4, 2, HD, 256), bf16),
            jax.ShapeDtypeStruct((4, 4, 2, 2, 256), f32),
        ),
        in_specs=[pl.BlockSpec(memory_space=pltpu.SMEM), vmem, vmem, vmem],
        out_specs=(vmem, vmem),
        scratch_shapes=[pltpu.VMEM((2 * SLOTS, 256), f32), pltpu.VMEM((2 * SLOTS, 256), f32)],
        compiler_params=pltpu.CompilerParams(vmem_limit_bytes=VMEM_LIMIT),
        name="attention",
    )(offset, q, k, vt)


def merge(parts):
    top = parts[0][1]
    for _, m, _ in parts[1:]:
        top = jnp.maximum(top, m)
    numer, denom = None, None
    for o, m, l in parts:
        factor = jnp.exp2(m - top)
        o = o.astype(f32) * factor
        l = l * factor
        numer = o if numer is None else numer + o
        denom = l if denom is None else denom + l
    return numer, top, denom


def reduce_kernel(
    o_ref, m_ref, w_ref, out_ref,
    w, own1, ownm, in1, inm1, mid, midm, in2, inm2, att, half, part, inx,
    wsem, lsem, s1, r1, s1m, r1m, s2, r2, s2m, r2m, ps, pr, xs, xr,
):
    seq, head, z, y, c = place()
    p = 1 - c
    partner = dev(z, y, p, head)
    weights = pltpu.make_async_copy(w_ref, w, wsem)
    weights.start()
    peers = [partner]
    for d in (1, 2, 3):
        peers.append(dev(z, (y + d) % 4, c, head))
        peers.append(dev((z + d) % 4, y, c, head))
        peers.append((seq, (head + d) % 4))

    locals_ = [
        pltpu.make_async_copy(o_ref.at[z, :, 0], own1.at[0], lsem.at[0]),
        pltpu.make_async_copy(o_ref.at[:, y, 1], own1.at[1], lsem.at[1]),
        pltpu.make_async_copy(m_ref.at[z, :, 0], ownm.at[0], lsem.at[2]),
        pltpu.make_async_copy(m_ref.at[:, y, 1], ownm.at[1], lsem.at[3]),
    ]
    for copy in locals_:
        copy.start()
    enter(peers)

    first = []
    for d in (2, 1, 3):
        zt, yt = (z + d) % 4, (y + d) % 4
        for copy in (
            remote(m_ref.at[zt, :, 0], inm1.at[0, d - 1], s1m.at[0, d - 1], r1m.at[0, d - 1], dev(zt, y, c, head)),
            remote(m_ref.at[:, yt, 1], inm1.at[1, d - 1], s1m.at[1, d - 1], r1m.at[1, d - 1], dev(z, yt, c, head)),
            remote(o_ref.at[zt, :, 0], in1.at[0, d - 1], s1.at[0, d - 1], r1.at[0, d - 1], dev(zt, y, c, head)),
            remote(o_ref.at[:, yt, 1], in1.at[1, d - 1], s1.at[1, d - 1], r1.at[1, d - 1], dev(z, yt, c, head)),
        ):
            copy.start()
            first.append(copy)
    for copy in locals_:
        copy.wait()
    for copy in first:
        copy.wait()

    def sum_first(i, _):
        for g in (0, 1):
            parts = [(own1[g, i], ownm[g, i, 0:1, :], ownm[g, i, 1:2, :])]
            for d in range(3):
                parts.append((in1[g, d, i], inm1[g, d, i, 0:1, :], inm1[g, d, i, 1:2, :]))
            numer, top, denom = merge(parts)
            mid[g, i] = numer.astype(bf16)
            midm[g, i, 0:1, :] = top
            midm[g, i, 1:2, :] = denom
        return 0

    lax.fori_loop(0, 4, sum_first, 0)
    second = []
    for d in (2, 1, 3):
        zt, yt = (z + d) % 4, (y + d) % 4
        for copy in (
            remote(midm.at[0, yt], inm2.at[0, d - 1], s2m.at[0, d - 1], r2m.at[0, d - 1], dev(z, yt, c, head)),
            remote(midm.at[1, zt], inm2.at[1, d - 1], s2m.at[1, d - 1], r2m.at[1, d - 1], dev(zt, y, c, head)),
            remote(mid.at[0, yt], in2.at[0, d - 1], s2.at[0, d - 1], r2.at[0, d - 1], dev(z, yt, c, head)),
            remote(mid.at[1, zt], in2.at[1, d - 1], s2.at[1, d - 1], r2.at[1, d - 1], dev(zt, y, c, head)),
        ):
            copy.start()
            second.append(copy)
    for copy in second:
        copy.wait()
    for g in (0, 1):
        me = y if g == 0 else z
        parts = [(mid[g, me], midm[g, me, 0:1, :], midm[g, me, 1:2, :])]
        for d in range(3):
            parts.append((in2[g, d], inm2[g, d, 0:1, :], inm2[g, d, 1:2, :]))
        numer, _, denom = merge(parts)
        done = numer / denom
        for h in (0, 1):
            rows = done[:, h * HD : (h + 1) * HD].T.astype(bf16)
            cols = slice((g * 2 + h) * HD, (g * 2 + h + 1) * HD)
            half[0, :, cols] = rows[:ROWS]
            half[1, :, cols] = rows[ROWS:]

    swap = remote(half.at[p], att.at[c], ps, pr, partner)
    swap.start()
    weights.wait()
    swap.wait()
    lhs = jnp.concatenate(
        [
            jnp.where(c == 0, half[0], att[0]),
            jnp.where(c == 0, att[1], half[1]),
        ],
        axis=1,
    )
    cols = 1152
    sends = []
    for d in (2, 1, 3, 0):
        target = (head + d) % 4
        block = jnp.dot(
            lhs, w[:, pl.ds(pl.multiple_of(target * cols, HD), cols)], preferred_element_type=f32
        )
        if d:
            part[d - 1] = block.astype(bf16)
            copy = remote(part.at[d - 1], inx.at[d - 1], xs.at[d - 1], xr.at[d - 1], (seq, target))
            copy.start()
            sends.append(copy)
        else:
            total = block
    for copy in sends:
        copy.wait()
    out_ref[...] = total + (
        (inx[0].astype(f32) + inx[1].astype(f32)) + inx[2].astype(f32)
    )


def reduction(o, m, weight):
    dma = pltpu.SemaphoreType.DMA
    hbm = pl.BlockSpec(memory_space=pl.ANY)
    return pl.pallas_call(
        reduce_kernel,
        out_shape=jax.ShapeDtypeStruct((ROWS, 1152), f32),
        in_specs=[hbm, hbm, hbm],
        out_specs=pl.BlockSpec(memory_space=pltpu.VMEM),
        scratch_shapes=[
            pltpu.VMEM((1024, 4608), bf16),
            pltpu.VMEM((2, 4, HD, 256), bf16),
            pltpu.VMEM((2, 4, 2, 256), f32),
            pltpu.VMEM((2, 3, 4, HD, 256), bf16),
            pltpu.VMEM((2, 3, 4, 2, 256), f32),
            pltpu.VMEM((2, 4, HD, 256), bf16),
            pltpu.VMEM((2, 4, 2, 256), f32),
            pltpu.VMEM((2, 3, HD, 256), bf16),
            pltpu.VMEM((2, 3, 2, 256), f32),
            pltpu.VMEM((2, ROWS, 512), bf16),
            pltpu.VMEM((2, ROWS, 512), bf16),
            pltpu.VMEM((3, ROWS, 1152), bf16),
            pltpu.VMEM((3, ROWS, 1152), bf16),
            dma,
            dma((4,)),
            dma((2, 3)),
            dma((2, 3)),
            dma((2, 3)),
            dma((2, 3)),
            dma((2, 3)),
            dma((2, 3)),
            dma((2, 3)),
            dma((2, 3)),
            dma,
            dma,
            dma((3,)),
            dma((3,)),
        ],
        compiler_params=pltpu.CompilerParams(
            collective_id=1, has_side_effects=True, vmem_limit_bytes=VMEM_LIMIT
        ),
        name="reduction",
    )(o, m, weight)


def shards(queries, keys, values, kv_len, causal_offset, out_weight):
    q, k, vt = gather(
        kv_len,
        queries.reshape(ROWS * 8, HD),
        keys.reshape(SLOTS * 4, HD),
        values.reshape(SLOTS * 4, HD),
    )
    o, m = attention(causal_offset, q, k, vt)
    return reduction(o, m, out_weight)


def solution(mesh):
    placed = (
        P("seq", "head", None),
        P("seq", "head", None),
        P("seq", "head", None),
        P("seq"),
        P(),
        P("head", None),
    )
    return jax.shard_map(
        shards, mesh=mesh, in_specs=placed, out_specs=P("seq", "head"), check_vma=False
    )
```

```python
import math

import jax
import jax.numpy as jnp
from jax import lax
from jax.experimental import pallas as pl
from jax.experimental.pallas import tpu as pltpu
from jax.sharding import PartitionSpec as P

bf16 = jnp.bfloat16
f32 = jnp.float32
MESH = pl.DeviceIdType.MESH
score_scale = math.log2(math.e) / 12.0
masked_score = -1e30
HD = 128
ROWS = 64
SLOTS = 2048
VROWS = 144
CH = 256
COLS = 1152
BLOCK = 256
BLOCKS = SLOTS // BLOCK


def remote(src, dst, send_sem, recv_sem, device):
    return pltpu.make_async_remote_copy(
        src_ref=src,
        dst_ref=dst,
        send_sem=send_sem,
        recv_sem=recv_sem,
        device_id=device,
        device_id_type=MESH,
    )


def merge(parts):
    top = parts[0][1]
    for _, m, _ in parts[1:]:
        top = jnp.maximum(top, m)
    numer, denom = None, None
    for o, m, l in parts:
        factor = jnp.exp2(m - top)
        o = o.astype(f32) * factor
        l = l * factor
        numer = o if numer is None else numer + o
        denom = l if denom is None else denom + l
    return numer, top, denom


def kernel(
    len_ref, off_ref, q_hbm, k_hbm, v_hbm, w_hbm, out_ref,
    q_raw, k_raw, v_raw, w, wide, qs, ks, vs, kp, vp, qg, s0, s1, tops,
    o_own, m_own, in1, inm1, mid, midm, in2, inm2, half, att, part, inx,
    lsem, kl, vl, psend, precv, ysend, yrecv, zsend, zrecv, fsend, frecv,
    ksend, krecv, vsend, vrecv, s1s, s1r, s1ms, s1mr, s2s, s2r, s2ms, s2mr, as_, ar, xs, xr,
):
    seq = lax.axis_index("seq")
    head = lax.axis_index("head")
    z, y, c = seq // 8, (seq // 2) % 4, seq % 2
    p = 1 - c

    def dev(zt, yt, core):
        return ((zt * 4 + yt) * 2 + core, head)

    def ahead(index, d):
        return lax.rem(index + d, 4)

    partner = dev(z, y, p)

    load_q = pltpu.make_async_copy(q_hbm, q_raw, lsem.at[0])
    load_w = pltpu.make_async_copy(w_hbm, w, lsem.at[1])

    def load_kv(b):
        rows = pl.ds(pl.multiple_of(b * BLOCK * 4, BLOCK * 4), BLOCK * 4)
        return (
            pltpu.make_async_copy(k_hbm.at[rows], k_raw.at[rows], kl.at[b]),
            pltpu.make_async_copy(v_hbm.at[rows], v_raw.at[rows], vl.at[b]),
        )

    load_q.start()
    for b in range(BLOCKS):
        for copy in load_kv(b):
            copy.start()
    load_w.start()

    peers = [partner]
    for d in (1, 2, 3):
        for core in (0, 1):
            peers.append(dev(z, ahead(y, d), core))
            peers.append(dev(ahead(z, d), y, core))
        peers.append((seq, ahead(head, d)))
    barrier = pltpu.get_barrier_semaphore()
    for peer in peers:
        pl.semaphore_signal(barrier, inc=1, device_id=peer, device_id_type=MESH)

    load_q.wait()
    wide[0 : ROWS * 8, :] = q_raw[...].astype(f32)
    for h in range(8):
        qs[h] = wide[pl.ds(h, ROWS, stride=8), :].astype(bf16)
    qg[z, y, c] = qs[pl.ds(4 * c, 4)]

    length = len_ref[0]

    def prepare(b, _):
        for copy in load_kv(b):
            copy.wait()
        k0 = k_raw[0:8, :].astype(f32)
        rows = pl.ds(pl.multiple_of(b * BLOCK * 4, BLOCK * 4), BLOCK * 4)
        slots = pl.ds(pl.multiple_of(b * BLOCK, BLOCK), BLOCK)
        filled = lax.broadcasted_iota(jnp.int32, (BLOCK, HD), 0) + b * BLOCK < length
        wide[...] = k_raw[rows, :].astype(f32)
        for h in range(4):
            one = wide[pl.ds(h, BLOCK, stride=4), :]
            ks[h, slots, :] = jnp.where(filled, one, k0[h : h + 1, :]).astype(bf16)
        wide[...] = v_raw[rows, :].astype(f32)
        col = lax.broadcasted_iota(jnp.int32, (VROWS - HD, BLOCK), 1) + b * BLOCK
        row = lax.broadcasted_iota(jnp.int32, (VROWS - HD, BLOCK), 0)
        ones = jnp.where((col < length) & (row == 0), 1.0, 0.0).astype(bf16)
        for h in range(4):
            one = wide[pl.ds(h, BLOCK, stride=4), :]
            vs[h, 0:HD, slots] = jnp.where(filled, one, 0.0).T.astype(bf16)
            vs[h, HD:VROWS, slots] = ones
        return 0

    def swap_kv(b):
        slots = pl.ds(pl.multiple_of(b * BLOCK, BLOCK), BLOCK)
        return (
            remote(ks.at[pl.ds(2 * p, 2), slots], kp.at[:, slots], ksend.at[b], krecv.at[b], partner),
            remote(
                vs.at[pl.ds(2 * p, 2), :, slots], vp.at[:, :, slots], vsend.at[b], vrecv.at[b], partner
            ),
        )

    lax.fori_loop(0, BLOCKS // 2, prepare, 0)
    pl.semaphore_wait(barrier, len(peers))

    first = [remote(qs.at[pl.ds(4 * p, 4)], qg.at[z, y, c], psend, precv, partner)]
    for d in (1, 3, 2):
        for core in (0, 1):
            first.append(
                remote(
                    qs.at[pl.ds(4 * core, 2)], qg.at[z, y, c, pl.ds(0, 2)],
                    ysend.at[d - 1, core], yrecv.at[d - 1, c], dev(z, ahead(y, d), core),
                )
            )
            first.append(
                remote(
                    qs.at[pl.ds(4 * core + 2, 2)], qg.at[z, y, c, pl.ds(2, 2)],
                    zsend.at[d - 1, core], zrecv.at[d - 1, c], dev(ahead(z, d), y, core),
                )
            )
    for copy in first:
        copy.start()

    def start_swap(b, _):
        for copy in swap_kv(b):
            copy.start()
        return 0

    lax.fori_loop(0, BLOCKS // 2, start_swap, 0)
    lax.fori_loop(BLOCKS // 2, BLOCKS, prepare, 0)
    lax.fori_loop(BLOCKS // 2, BLOCKS, start_swap, 0)

    last_chip = (z == 3) & (y == 3)
    offset = off_ref[0] - 30 * SLOTS

    def queries_of(zq, yq, group):
        parts = [qg[zq, yq, core, group * 2 + h] for h in (0, 1) for core in (0, 1)]
        q = jnp.concatenate(parts, axis=0).astype(f32) * score_scale
        high = q.astype(bf16)
        low = (q - high.astype(f32)).astype(bf16)
        return jnp.concatenate([high, low], axis=1)

    def limit_of(zq, yq):
        lane = lax.broadcasted_iota(jnp.int32, (8, 256), 1) % HD
        return offset + (zq * 4 + yq) * HD + lane - lax.broadcasted_iota(jnp.int32, (8, 256), 0)

    def scores(qq, limit, group, shard, start, s_ref, m):
        rows = pl.ds(start, CH)
        k = ks[2 * c + group, rows, :] if shard == 0 else kp[group, rows, :]
        kk = jnp.concatenate([k, k], axis=1)
        s = lax.dot_general(kk, qq, (((1,), (1,)), ((), ())), preferred_element_type=f32)
        s = s.reshape(CH // 8, 8, 256)
        if limit is not None:
            first_key = start + SLOTS * (c if shard == 0 else p)
            room = limit - first_key
            s = jnp.stack(
                [jnp.where(room >= 8 * i, s[i], masked_score) for i in range(CH // 8)]
            )
        s_ref[pl.ds(shard * SLOTS + start, CH), :] = s.reshape(CH, 256)
        return jnp.maximum(m, jnp.max(s, axis=0))

    def weigh(s_ref, m_now, group, shard, start, acc):
        s = s_ref[pl.ds(shard * SLOTS + start, CH), :].reshape(CH // 8, 8, 256)
        prob = jnp.exp2(s - m_now[None]).reshape(CH, 256).astype(bf16)
        cols = pl.ds(start, CH)
        vt = vs[2 * c + group, :, cols] if shard == 0 else vp[group, :, cols]
        return acc + jnp.dot(vt, prob, preferred_element_type=f32)

    steps = [(shard, start) for shard in (0, 1) for start in range(0, SLOTS, CH)]

    def tiles(new, cur, causal):
        m = jnp.full((8, 256), masked_score, f32)
        if new is not None:
            qq = queries_of(new[0], new[1], new[2])
            limit = limit_of(new[0], new[1]) if causal else None
        acc = jnp.zeros((VROWS, 256), f32)
        if cur is not None:
            m_now = tops[cur[0]]
        for shard, start in steps:
            if new is not None:
                s_ref = s1 if new[2] else s0
                m = scores(qq, limit, new[2], shard, start, s_ref, m)
            if cur is not None:
                s_ref = s1 if cur[0] else s0
                acc = weigh(s_ref, m_now, cur[0], shard, start, acc)
        if cur is not None:
            group, d, i = cur
            o_own[group, d, i] = acc[:HD].astype(bf16)
            m_own[group, d, i, 0:1, :] = m_now[0:1]
            m_own[group, d, i, 1:2, :] = acc[HD : HD + 1]
        if new is not None:
            tops[new[2]] = jnp.broadcast_to(jnp.max(m, axis=0, keepdims=True), (8, 256))

    def both(new, cur):
        @pl.when(jnp.logical_not(last_chip))
        def _():
            tiles(new, cur, False)

        @pl.when(last_chip)
        def _():
            tiles(new, cur, True)

    def tile0(d, i):
        return ahead(z, d), ahead(y, i), 0

    def tile1(d, i):
        return ahead(z, i), ahead(y, d), 1

    def sends(group, d, i):
        target = dev(ahead(z, d), y, c) if group == 0 else dev(z, ahead(y, d), c)
        return (
            remote(
                m_own.at[group, d, i], inm1.at[group, d - 1, i],
                s1ms.at[group, d - 1, i], s1mr.at[group, d - 1, i], target,
            ),
            remote(
                o_own.at[group, d, i], in1.at[group, d - 1, i],
                s1s.at[group, d - 1, i], s1r.at[group, d - 1, i], target,
            ),
        )

    first[0].wait_recv()
    for d in (1, 2, 3):
        for core in (0, 1):
            remote(
                qs.at[pl.ds(0, 2)], qg.at[z, ahead(y, 4 - d), core, pl.ds(0, 2)],
                ysend.at[d - 1, core], yrecv.at[d - 1, core], partner,
            ).wait_recv()
            remote(
                qs.at[pl.ds(0, 2)], qg.at[ahead(z, 4 - d), y, core, pl.ds(2, 2)],
                zsend.at[d - 1, core], zrecv.at[d - 1, core], partner,
            ).wait_recv()

    second = []
    for d in (3, 1, 2):
        src = qg.at[z, :, :, pl.ds(0, 2)]
        second.append(remote(src, src, fsend.at[0, d - 1], frecv.at[0, d - 1], dev(ahead(z, 4 - d), y, c)))
        src = qg.at[:, y, :, pl.ds(2, 2)]
        second.append(remote(src, src, fsend.at[1, d - 1], frecv.at[1, d - 1], dev(z, ahead(y, 4 - d), c)))
    for copy in second:
        copy.start()

    def wait_swap(b, _):
        for copy in swap_kv(b):
            copy.wait()
        return 0

    lax.fori_loop(0, BLOCKS, wait_swap, 0)
    both(tile0(0, 0), None)

    def body(u, _):
        d, i = u // 4, lax.rem(u, 4)
        both(tile1(d, i), (0, d, i))

        @pl.when(u > 4)
        def _():
            for copy in sends(1, (u - 1) // 4, lax.rem(u - 1, 4)):
                copy.start()

        @pl.when(i == 3)
        def _():
            src = qg.at[ahead(z, d + 1), :, :, pl.ds(0, 2)]
            remote(src, src, fsend.at[0, d], frecv.at[0, d], partner).wait_recv()
            src = qg.at[:, ahead(y, d + 1), :, pl.ds(2, 2)]
            remote(src, src, fsend.at[1, d], frecv.at[1, d], partner).wait_recv()

        both(tile0((u + 1) // 4, lax.rem(u + 1, 4)), (1, d, i))

        @pl.when(d > 0)
        def _():
            for copy in sends(0, d, i):
                copy.start()

        return 0

    lax.fori_loop(0, 15, body, 0)
    both(tile1(3, 3), (0, 3, 3))
    for copy in sends(1, 3, 2):
        copy.start()
    both(None, (1, 3, 3))
    for copy in sends(0, 3, 3):
        copy.start()
    for copy in sends(1, 3, 3):
        copy.start()

    for copy in first + second:
        copy.wait_send()
    for d in (1, 2, 3):
        for i in range(4):
            for group in (0, 1):
                for copy in sends(group, d, i):
                    copy.wait()

    def sum_first(i, _):
        for g in (0, 1):
            parts = [(o_own[g, 0, i], m_own[g, 0, i, 0:1, :], m_own[g, 0, i, 1:2, :])]
            for d in range(3):
                parts.append((in1[g, d, i], inm1[g, d, i, 0:1, :], inm1[g, d, i, 1:2, :]))
            numer, top, denom = merge(parts)
            mid[g, i] = numer.astype(bf16)
            midm[g, i, 0:1, :] = top
            midm[g, i, 1:2, :] = denom
        return 0

    lax.fori_loop(0, 4, sum_first, 0)
    third = []
    for i in (2, 1, 3):
        for g in (0, 1):
            target = dev(z, ahead(y, i), c) if g == 0 else dev(ahead(z, i), y, c)
            third.append(remote(midm.at[g, i], inm2.at[g, i - 1], s2ms.at[g, i - 1], s2mr.at[g, i - 1], target))
            third.append(remote(mid.at[g, i], in2.at[g, i - 1], s2s.at[g, i - 1], s2r.at[g, i - 1], target))
    for copy in third:
        copy.start()
    for copy in third:
        copy.wait()
    for g in (0, 1):
        parts = [(mid[g, 0], midm[g, 0, 0:1, :], midm[g, 0, 1:2, :])]
        for i in range(3):
            parts.append((in2[g, i], inm2[g, i, 0:1, :], inm2[g, i, 1:2, :]))
        numer, _, denom = merge(parts)
        done = numer / denom
        for h in (0, 1):
            rows = done[:, h * HD : (h + 1) * HD].T.astype(bf16)
            cols = slice((g * 2 + h) * HD, (g * 2 + h + 1) * HD)
            half[0, :, cols] = rows[:ROWS]
            half[1, :, cols] = rows[ROWS:]

    swap = remote(half.at[p], att.at[c], as_, ar, partner)
    swap.start()
    load_w.wait()
    swap.wait()
    lhs = jnp.concatenate(
        [jnp.where(c == 0, half[0], att[0]), jnp.where(c == 0, att[1], half[1])], axis=1
    )
    fourth = []
    for d in (2, 1, 3, 0):
        target = ahead(head, d)
        cols = pl.ds(pl.multiple_of(target * COLS, HD), COLS)
        block = jnp.dot(lhs, w[:, cols], preferred_element_type=f32)
        if d:
            part[d - 1] = block.astype(bf16)
            copy = remote(part.at[d - 1], inx.at[d - 1], xs.at[d - 1], xr.at[d - 1], (seq, target))
            copy.start()
            fourth.append(copy)
        else:
            total = block
    for copy in fourth:
        copy.wait()
    out_ref[...] = total + ((inx[0].astype(f32) + inx[1].astype(f32)) + inx[2].astype(f32))


def shards(queries, keys, values, kv_len, causal_offset, out_weight):
    dma = pltpu.SemaphoreType.DMA
    hbm = pl.BlockSpec(memory_space=pl.ANY)
    smem = pl.BlockSpec(memory_space=pltpu.SMEM)

    def vmem(*shape, dtype=bf16):
        return pltpu.VMEM(shape, dtype)

    return pl.pallas_call(
        kernel,
        out_shape=jax.ShapeDtypeStruct((ROWS, COLS), f32),
        in_specs=[smem, smem, hbm, hbm, hbm, hbm],
        out_specs=pl.BlockSpec(memory_space=pltpu.VMEM),
        scratch_shapes=[
            vmem(ROWS * 8, HD),
            vmem(SLOTS * 4, HD),
            vmem(SLOTS * 4, HD),
            vmem(1024, 4608),
            vmem(BLOCK * 4, HD, dtype=f32),
            vmem(8, ROWS, HD),
            vmem(4, SLOTS, HD),
            vmem(4, VROWS, SLOTS),
            vmem(2, SLOTS, HD),
            vmem(2, VROWS, SLOTS),
            vmem(4, 4, 2, 4, ROWS, HD),
            vmem(2 * SLOTS, 256, dtype=f32),
            vmem(2 * SLOTS, 256, dtype=f32),
            vmem(2, 8, 256, dtype=f32),
            vmem(2, 4, 4, HD, 256),
            vmem(2, 4, 4, 2, 256, dtype=f32),
            vmem(2, 3, 4, HD, 256),
            vmem(2, 3, 4, 2, 256, dtype=f32),
            vmem(2, 4, HD, 256),
            vmem(2, 4, 2, 256, dtype=f32),
            vmem(2, 3, HD, 256),
            vmem(2, 3, 2, 256, dtype=f32),
            vmem(2, ROWS, 512),
            vmem(2, ROWS, 512),
            vmem(3, ROWS, COLS),
            vmem(3, ROWS, COLS),
            dma((2,)), dma((BLOCKS,)), dma((BLOCKS,)),
            dma, dma,
            dma((3, 2)), dma((3, 2)), dma((3, 2)), dma((3, 2)),
            dma((2, 3)), dma((2, 3)),
            dma((BLOCKS,)), dma((BLOCKS,)), dma((BLOCKS,)), dma((BLOCKS,)),
            dma((2, 3, 4)), dma((2, 3, 4)), dma((2, 3, 4)), dma((2, 3, 4)),
            dma((2, 3)), dma((2, 3)), dma((2, 3)), dma((2, 3)),
            dma, dma,
            dma((3,)), dma((3,)),
        ],
        compiler_params=pltpu.CompilerParams(
            collective_id=0, has_side_effects=True, vmem_limit_bytes=60 * 2**20
        ),
        name="attend",
    )(
        kv_len,
        causal_offset,
        queries.reshape(ROWS * 8, HD),
        keys.reshape(SLOTS * 4, HD),
        values.reshape(SLOTS * 4, HD),
        out_weight,
    )


def solution(mesh):
    placed = (
        P("seq", "head", None),
        P("seq", "head", None),
        P("seq", "head", None),
        P("seq"),
        P(),
        P("head", None),
    )
    return jax.shard_map(
        shards, mesh=mesh, in_specs=placed, out_specs=P("seq", "head"), check_vma=False
    )
```

```python
import math

import jax
import jax.numpy as jnp
from jax import lax
from jax.experimental import pallas as pl
from jax.experimental.pallas import tpu as pltpu
from jax.sharding import PartitionSpec as P

bf16 = jnp.bfloat16
f32 = jnp.float32
MESH = pl.DeviceIdType.MESH
score_scale = math.log2(math.e) / 12.0
masked_score = -1e30
HD = 128
ROWS = 64
SLOTS = 2048
VROWS = 144
CH = 256
COLS = 1152
BLOCK = 256
BLOCKS = SLOTS // BLOCK


def remote(src, dst, send_sem, recv_sem, device):
    return pltpu.make_async_remote_copy(
        src_ref=src,
        dst_ref=dst,
        send_sem=send_sem,
        recv_sem=recv_sem,
        device_id=device,
        device_id_type=MESH,
    )


def merge(parts):
    top = parts[0][1]
    for _, m, _ in parts[1:]:
        top = jnp.maximum(top, m)
    numer, denom = None, None
    for o, m, l in parts:
        factor = jnp.exp2(m - top)
        o = o.astype(f32) * factor
        l = l * factor
        numer = o if numer is None else numer + o
        denom = l if denom is None else denom + l
    return numer, top, denom


def kernel(
    len_ref, off_ref, q_hbm, k_hbm, v_hbm, w_hbm, out_ref,
    q_raw, k_raw, v_raw, w_vmem, wide, qs, ks, vs, kp, vp, qg, s0, s1, tops,
    o_own, m_own, in1, inm1, mid, midm, in2, inm2, lhs, part, total, inx,
    lsem, kl, vl, psend, precv, ysend, yrecv, zsend, zrecv, fsend, frecv,
    ksend, krecv, vsend, vrecv, s1s, s1r, s1ms, s1mr, s2s, s2r, s2ms, s2mr, xs, xr,
):
    seq = lax.axis_index("seq")
    head = lax.axis_index("head")
    z, y, c = seq // 8, (seq // 2) % 4, seq % 2
    p = 1 - c

    def dev(zt, yt, core):
        return ((zt * 4 + yt) * 2 + core, head)

    def ahead(index, d):
        return lax.rem(index + d, 4)

    partner = dev(z, y, p)

    load_q = pltpu.make_async_copy(q_hbm, q_raw, lsem.at[0])
    load_w = pltpu.make_async_copy(w_hbm, w_vmem, lsem.at[1])

    def load_kv(b):
        rows = pl.ds(pl.multiple_of(b * BLOCK * 4, BLOCK * 4), BLOCK * 4)
        return (
            pltpu.make_async_copy(k_hbm.at[rows], k_raw.at[rows], kl.at[b]),
            pltpu.make_async_copy(v_hbm.at[rows], v_raw.at[rows], vl.at[b]),
        )

    load_q.start()
    for b in range(BLOCKS):
        for copy in load_kv(b):
            copy.start()

    peers = [partner]
    for d in (1, 2, 3):
        for core in (0, 1):
            peers.append(dev(z, ahead(y, d), core))
            peers.append(dev(ahead(z, d), y, core))
        peers.append((seq, ahead(head, d)))
    barrier = pltpu.get_barrier_semaphore()
    for peer in peers:
        pl.semaphore_signal(barrier, inc=1, device_id=peer, device_id_type=MESH)

    load_q.wait()
    wide[0 : ROWS * 8, :] = q_raw[...].astype(f32)
    for h in range(8):
        qs[h] = wide[pl.ds(h, ROWS, stride=8), :].astype(bf16)
    qg[z, y, c] = qs[pl.ds(4 * c, 4)]

    length = len_ref[0]

    def prepare(b, _):
        for copy in load_kv(b):
            copy.wait()
        k0 = k_raw[0:8, :].astype(f32)
        rows = pl.ds(pl.multiple_of(b * BLOCK * 4, BLOCK * 4), BLOCK * 4)
        slots = pl.ds(pl.multiple_of(b * BLOCK, BLOCK), BLOCK)
        filled = lax.broadcasted_iota(jnp.int32, (BLOCK, HD), 0) + b * BLOCK < length
        wide[...] = k_raw[rows, :].astype(f32)
        for h in range(4):
            one = wide[pl.ds(h, BLOCK, stride=4), :]
            ks[h, slots, :] = jnp.where(filled, one, k0[h : h + 1, :]).astype(bf16)
        wide[...] = v_raw[rows, :].astype(f32)
        col = lax.broadcasted_iota(jnp.int32, (VROWS - HD, BLOCK), 1) + b * BLOCK
        row = lax.broadcasted_iota(jnp.int32, (VROWS - HD, BLOCK), 0)
        ones = jnp.where((col < length) & (row == 0), 1.0, 0.0).astype(bf16)
        for h in range(4):
            one = wide[pl.ds(h, BLOCK, stride=4), :]
            vs[h, 0:HD, slots] = jnp.where(filled, one, 0.0).T.astype(bf16)
            vs[h, HD:VROWS, slots] = ones
        return 0

    def swap_kv(b):
        slots = pl.ds(pl.multiple_of(b * BLOCK, BLOCK), BLOCK)
        return (
            remote(ks.at[pl.ds(2 * p, 2), slots], kp.at[:, slots], ksend.at[b], krecv.at[b], partner),
            remote(
                vs.at[pl.ds(2 * p, 2), :, slots], vp.at[:, :, slots], vsend.at[b], vrecv.at[b], partner
            ),
        )

    lax.fori_loop(0, BLOCKS // 2, prepare, 0)
    pl.semaphore_wait(barrier, len(peers))

    first = [remote(qs.at[pl.ds(4 * p, 4)], qg.at[z, y, c], psend, precv, partner)]
    for d in (1, 3, 2):
        for core in (0, 1):
            first.append(
                remote(
                    qs.at[pl.ds(4 * core, 2)], qg.at[z, y, c, pl.ds(0, 2)],
                    ysend.at[d - 1, core], yrecv.at[d - 1, c], dev(z, ahead(y, d), core),
                )
            )
            first.append(
                remote(
                    qs.at[pl.ds(4 * core + 2, 2)], qg.at[z, y, c, pl.ds(2, 2)],
                    zsend.at[d - 1, core], zrecv.at[d - 1, c], dev(ahead(z, d), y, core),
                )
            )
    for copy in first:
        copy.start()

    def start_swap(b, _):
        for copy in swap_kv(b):
            copy.start()
        return 0

    lax.fori_loop(0, BLOCKS // 2, start_swap, 0)
    lax.fori_loop(BLOCKS // 2, BLOCKS, prepare, 0)
    lax.fori_loop(BLOCKS // 2, BLOCKS, start_swap, 0)
    load_w.start()

    last_chip = (z == 3) & (y == 3)
    offset = off_ref[0] - 30 * SLOTS

    def chips(group, d, j):
        if group == 0:
            return [(ahead(z, d), ahead(y, 2 * j + e)) for e in (0, 1)]
        return [(ahead(z, 2 * j + e), ahead(y, d)) for e in (0, 1)]

    def queries_of(group, w, d, j):
        parts = [qg[zq, yq, w, group * 2 + h] for zq, yq in chips(group, d, j) for h in (0, 1)]
        q = jnp.concatenate(parts, axis=0).astype(f32) * score_scale
        high = q.astype(bf16)
        low = (q - high.astype(f32)).astype(bf16)
        return jnp.concatenate([high, low], axis=1)

    def limit_of(group, w, d, j):
        lane = lax.broadcasted_iota(jnp.int32, (8, 256), 1)
        (za, ya), (zb, yb) = chips(group, d, j)
        chip = jnp.where(lane < HD, za * 4 + ya, zb * 4 + yb)
        row = chip * HD + w * ROWS + lane % ROWS
        return offset + row - lax.broadcasted_iota(jnp.int32, (8, 256), 0)

    def scores(qq, limit, group, shard, start, s_ref, m):
        rows = pl.ds(start, CH)
        k = ks[2 * c + group, rows, :] if shard == 0 else kp[group, rows, :]
        kk = jnp.concatenate([k, k], axis=1)
        s = lax.dot_general(kk, qq, (((1,), (1,)), ((), ())), preferred_element_type=f32)
        s = s.reshape(CH // 8, 8, 256)
        if limit is not None:
            first_key = start + SLOTS * (c if shard == 0 else p)
            room = limit - first_key
            s = jnp.stack(
                [jnp.where(room >= 8 * i, s[i], masked_score) for i in range(CH // 8)]
            )
        s_ref[pl.ds(shard * SLOTS + start, CH), :] = s.reshape(CH, 256)
        return jnp.maximum(m, jnp.max(s, axis=0))

    def weigh(s_ref, m_now, group, shard, start, acc):
        s = s_ref[pl.ds(shard * SLOTS + start, CH), :].reshape(CH // 8, 8, 256)
        prob = jnp.exp2(s - m_now[None]).reshape(CH, 256).astype(bf16)
        cols = pl.ds(start, CH)
        vt = vs[2 * c + group, :, cols] if shard == 0 else vp[group, :, cols]
        return acc + jnp.dot(vt, prob, preferred_element_type=f32)

    steps = [(shard, start) for shard in (0, 1) for start in range(0, SLOTS, CH)]

    def tiles(new, cur, causal):
        m = jnp.full((8, 256), masked_score, f32)
        if new is not None:
            qq = queries_of(*new)
            limit = limit_of(*new) if causal else None
        acc = jnp.zeros((VROWS, 256), f32)
        if cur is not None:
            m_now = tops[cur[0]]
        for shard, start in steps:
            if new is not None:
                s_ref = s1 if new[0] else s0
                m = scores(qq, limit, new[0], shard, start, s_ref, m)
            if cur is not None:
                s_ref = s1 if cur[0] else s0
                acc = weigh(s_ref, m_now, cur[0], shard, start, acc)
        if cur is not None:
            group, w, d, j = cur
            o_own[group, w, d, j] = acc[:HD].astype(bf16)
            m_own[group, w, d, j, 0:1, :] = m_now[0:1]
            m_own[group, w, d, j, 1:2, :] = acc[HD : HD + 1]
        if new is not None:
            tops[new[0]] = jnp.broadcast_to(jnp.max(m, axis=0, keepdims=True), (8, 256))

    def both(new, cur):
        @pl.when(jnp.logical_not(last_chip))
        def _():
            tiles(new, cur, False)

        @pl.when(last_chip)
        def _():
            tiles(new, cur, True)

    def step(u):
        w = u // 8
        k = lax.rem(lax.rem(u, 8) // 2 + w, 4)
        return w, lax.rem(k * (k + 1) // 2, 4), lax.rem(u, 2)

    def sends(group, w, d, j):
        target = dev(ahead(z, d), y, c) if group == 0 else dev(z, ahead(y, d), c)
        slot = (group, w, d - 1, j)
        return (
            remote(m_own.at[group, w, d, j], inm1.at[slot], s1ms.at[slot], s1mr.at[slot], target),
            remote(o_own.at[group, w, d, j], in1.at[slot], s1s.at[slot], s1r.at[slot], target),
        )

    def send_tile(group, u):
        w, d, j = step(u)

        @pl.when(d > 0)
        def _():
            for copy in sends(group, w, d, j):
                copy.start()

    def passes(group, w, i):
        if i == 0:
            target = partner
        else:
            target = dev(z, ahead(y, i), w) if group == 0 else dev(ahead(z, i), y, w)
        return (
            remote(
                midm.at[group, w, i], inm2.at[c, group, i],
                s2ms.at[group, w, i], s2mr.at[c, group, i], target,
            ),
            remote(
                mid.at[group, w, i], in2.at[c, group, i],
                s2s.at[group, w, i], s2r.at[c, group, i], target,
            ),
        )

    def sum_first(group, w, j):
        for d in (1, 2, 3):
            for copy in sends(group, w, d, j):
                copy.wait_recv()
        parts = [
            (o_own[group, w, 0, j], m_own[group, w, 0, j, 0:1, :], m_own[group, w, 0, j, 1:2, :])
        ]
        for d in range(3):
            parts.append(
                (in1[group, w, d, j], inm1[group, w, d, j, 0:1, :], inm1[group, w, d, j, 1:2, :])
            )
        numer, top, denom = merge(parts)
        for e in (0, 1):
            i = 2 * j + e
            lanes = slice(e * HD, (e + 1) * HD)
            mid[group, w, i] = numer[:, lanes].astype(bf16)
            midm[group, w, i, 0:1, :] = top[:, lanes]
            midm[group, w, i, 1:2, :] = denom[:, lanes]
        for e in (1, 0):
            i = 2 * j + e
            if i:
                for copy in passes(group, w, i):
                    copy.start()
            else:

                @pl.when(c != w)
                def _():
                    for copy in passes(group, w, 0):
                        copy.start()

                @pl.when(c == w)
                def _():
                    in2[c, group, 0] = mid[group, w, 0]
                    inm2[c, group, 0] = midm[group, w, 0]

    def exchange(d):
        return remote(
            part.at[d - 1], inx.at[d - 1], xs.at[d - 1], xr.at[d - 1], (seq, ahead(head, d))
        )

    def project(w):
        for group in (0, 1):
            for source in (0, 1):
                for i in range(4):
                    if i or source != w:
                        slot = (source, group, i)
                        remote(
                            midm.at[group, w, i], inm2.at[slot],
                            s2ms.at[group, w, i], s2mr.at[slot], partner,
                        ).wait_recv()
                        remote(
                            mid.at[group, w, i], in2.at[slot],
                            s2s.at[group, w, i], s2r.at[slot], partner,
                        ).wait_recv()
        for source in (0, 1):
            for group in (0, 1):
                parts = [
                    (
                        in2[source, group, i],
                        inm2[source, group, i, 0:1, :],
                        inm2[source, group, i, 1:2, :],
                    )
                    for i in range(4)
                ]
                numer, _, denom = merge(parts)
                rows = (numer / denom).T.astype(bf16)
                first_col = (source * 2 + group) * 2 * HD
                for h in (0, 1):
                    cols = slice(first_col + h * HD, first_col + (h + 1) * HD)
                    lhs[:, cols] = rows[h * ROWS : (h + 1) * ROWS]
        load_w.wait()
        left = lhs[...]
        for d in (2, 1, 3, 0):
            cols = pl.ds(pl.multiple_of(ahead(head, d) * COLS, HD), COLS)
            block = jnp.dot(left, w_vmem[:, cols], preferred_element_type=f32)
            if d:
                part[d - 1] = block.astype(bf16)
                exchange(d).start()
            else:
                total[...] = block

    def finish():
        for d in (1, 2, 3):
            exchange(d).wait()
        out_ref[...] = total[...] + (
            (inx[0].astype(f32) + inx[1].astype(f32)) + inx[2].astype(f32)
        )

    first[0].wait_recv()
    for d in (1, 2, 3):
        for core in (0, 1):
            remote(
                qs.at[pl.ds(0, 2)], qg.at[z, ahead(y, 4 - d), core, pl.ds(0, 2)],
                ysend.at[d - 1, core], yrecv.at[d - 1, core], partner,
            ).wait_recv()
            remote(
                qs.at[pl.ds(0, 2)], qg.at[ahead(z, 4 - d), y, core, pl.ds(2, 2)],
                zsend.at[d - 1, core], zrecv.at[d - 1, core], partner,
            ).wait_recv()

    def forward(group, w, d, back):
        if group == 0:
            src = qg.at[ahead(z, d) if back else z, :, w, pl.ds(0, 2)]
            target = dev(ahead(z, 4 - d), y, c)
        else:
            src = qg.at[:, ahead(y, d) if back else y, w, pl.ds(2, 2)]
            target = dev(z, ahead(y, 4 - d), c)
        slot = (group, w, d - 1)
        return remote(src, src, fsend.at[slot], frecv.at[slot], target)

    second = [forward(g, w, d, False) for w in (0, 1) for d in (1, 3, 2) for g in (0, 1)]
    for copy in second:
        copy.start()

    def wait_swap(b, _):
        for copy in swap_kv(b):
            copy.wait()
        return 0

    lax.fori_loop(0, BLOCKS, wait_swap, 0)
    both((0, *step(0)), None)

    def body(u, _):
        both((1, *step(u)), (0, *step(u)))

        @pl.when(u > 0)
        def _():
            send_tile(1, u - 1)

        w, d, j = step(u + 1)

        @pl.when((j == 0) & (d > 0))
        def _():
            for group in (0, 1):
                forward(group, w, d, True).wait_recv()

        both((0, w, d, j), (1, *step(u)))
        send_tile(0, u)

        @pl.when(u == 10)
        def _():
            for j in (0, 1):
                for group in (0, 1):
                    sum_first(group, 0, j)

        @pl.when((u == 12) & (c == 0))
        def _():
            project(0)

        @pl.when(u == 14)
        def _():
            sum_first(0, 1, 0)
            sum_first(1, 1, 0)

        return 0

    lax.fori_loop(0, 15, body, 0)
    both((1, 1, 0, 1), (0, 1, 0, 1))
    sum_first(0, 1, 1)
    both(None, (1, 1, 0, 1))
    sum_first(1, 1, 1)

    @pl.when(c == 1)
    def _():
        project(1)

    for copy in first + second:
        copy.wait_send()
    for group in (0, 1):
        for w in (0, 1):
            for j in (0, 1):
                for d in (1, 2, 3):
                    for copy in sends(group, w, d, j):
                        copy.wait_send()
            for i in (1, 2, 3):
                for copy in passes(group, w, i):
                    copy.wait_send()

            @pl.when(c != w)
            def _():
                for copy in passes(group, w, 0):
                    copy.wait_send()

    finish()


def shards(queries, keys, values, kv_len, causal_offset, out_weight):
    dma = pltpu.SemaphoreType.DMA
    hbm = pl.BlockSpec(memory_space=pl.ANY)
    smem = pl.BlockSpec(memory_space=pltpu.SMEM)

    def vmem(*shape, dtype=bf16):
        return pltpu.VMEM(shape, dtype)

    return pl.pallas_call(
        kernel,
        out_shape=jax.ShapeDtypeStruct((ROWS, COLS), f32),
        in_specs=[smem, smem, hbm, hbm, hbm, hbm],
        out_specs=pl.BlockSpec(memory_space=pltpu.VMEM),
        scratch_shapes=[
            vmem(ROWS * 8, HD),
            vmem(SLOTS * 4, HD),
            vmem(SLOTS * 4, HD),
            vmem(1024, 4608),
            vmem(BLOCK * 4, HD, dtype=f32),
            vmem(8, ROWS, HD),
            vmem(4, SLOTS, HD),
            vmem(4, VROWS, SLOTS),
            vmem(2, SLOTS, HD),
            vmem(2, VROWS, SLOTS),
            vmem(4, 4, 2, 4, ROWS, HD),
            vmem(2 * SLOTS, 256, dtype=f32),
            vmem(2 * SLOTS, 256, dtype=f32),
            vmem(2, 8, 256, dtype=f32),
            vmem(2, 2, 4, 2, HD, 256),
            vmem(2, 2, 4, 2, 2, 256, dtype=f32),
            vmem(2, 2, 3, 2, HD, 256),
            vmem(2, 2, 3, 2, 2, 256, dtype=f32),
            vmem(2, 2, 4, HD, HD),
            vmem(2, 2, 4, 2, HD, dtype=f32),
            vmem(2, 2, 4, HD, HD),
            vmem(2, 2, 4, 2, HD, dtype=f32),
            vmem(ROWS, 1024),
            vmem(3, ROWS, COLS),
            vmem(ROWS, COLS, dtype=f32),
            vmem(3, ROWS, COLS),
            dma((2,)), dma((BLOCKS,)), dma((BLOCKS,)),
            dma, dma,
            dma((3, 2)), dma((3, 2)), dma((3, 2)), dma((3, 2)),
            dma((2, 2, 3)), dma((2, 2, 3)),
            dma((BLOCKS,)), dma((BLOCKS,)), dma((BLOCKS,)), dma((BLOCKS,)),
            dma((2, 2, 3, 2)), dma((2, 2, 3, 2)), dma((2, 2, 3, 2)), dma((2, 2, 3, 2)),
            dma((2, 2, 4)), dma((2, 2, 4)), dma((2, 2, 4)), dma((2, 2, 4)),
            dma((3,)), dma((3,)),
        ],
        compiler_params=pltpu.CompilerParams(
            collective_id=0, has_side_effects=True, vmem_limit_bytes=60 * 2**20
        ),
        name="attend",
    )(
        kv_len,
        causal_offset,
        queries.reshape(ROWS * 8, HD),
        keys.reshape(SLOTS * 4, HD),
        values.reshape(SLOTS * 4, HD),
        out_weight,
    )


def solution(mesh):
    placed = (
        P("seq", "head", None),
        P("seq", "head", None),
        P("seq", "head", None),
        P("seq"),
        P(),
        P("head", None),
    )
    return jax.shard_map(
        shards, mesh=mesh, in_specs=placed, out_specs=P("seq", "head"), check_vma=False
    )
```

```python
import math

import jax
import jax.numpy as jnp
from jax import lax
from jax.experimental import pallas as pl
from jax.experimental.pallas import tpu as pltpu
from jax.sharding import PartitionSpec as P

bf16 = jnp.bfloat16
f32 = jnp.float32
MESH = pl.DeviceIdType.MESH
score_scale = math.log2(math.e) / 12.0
masked_score = -1e30
HD = 128
ROWS = 64
SLOTS = 2048
VROWS = 144
COLS = 1152
BLOCK = 256
BLOCKS = SLOTS // BLOCK


def remote(src, dst, send_sem, recv_sem, device):
    return pltpu.make_async_remote_copy(
        src_ref=src,
        dst_ref=dst,
        send_sem=send_sem,
        recv_sem=recv_sem,
        device_id=device,
        device_id_type=MESH,
    )


def merge(parts):
    top = parts[0][1]
    for _, m, _ in parts[1:]:
        top = jnp.maximum(top, m)
    numer, denom = None, None
    for o, m, l in parts:
        factor = jnp.exp2(m - top)
        o = o.astype(f32) * factor
        l = l * factor
        numer = o if numer is None else numer + o
        denom = l if denom is None else denom + l
    return numer, top, denom


def kernel(
    len_ref, off_ref, q_hbm, k_hbm, v_hbm, w_hbm, out_ref,
    q_raw, k_raw, v_raw, w_vmem, wide, qs, ks, vs, kp, vp, qg, sa0, sa1, sb0, sb1, tops,
    o_own, m_own, in1, inm1, mid, midm, in2, inm2, lhs, part, total, inx,
    lsem, kl, vl, psend, precv, ysend, yrecv, zsend, zrecv, fsend, frecv,
    ksend, krecv, vsend, vrecv, s1s, s1r, s1ms, s1mr, s2s, s2r, s2ms, s2mr, xs, xr,
):
    seq = lax.axis_index("seq")
    head = lax.axis_index("head")
    z, y, c = seq // 8, (seq // 2) % 4, seq % 2
    p = 1 - c

    def dev(zt, yt, core):
        return ((zt * 4 + yt) * 2 + core, head)

    def ahead(index, d):
        return lax.rem(index + d, 4)

    partner = dev(z, y, p)

    load_q = pltpu.make_async_copy(q_hbm, q_raw, lsem.at[0])
    load_w = pltpu.make_async_copy(w_hbm, w_vmem, lsem.at[1])

    def load_kv(b):
        rows = pl.ds(pl.multiple_of(b * BLOCK * 4, BLOCK * 4), BLOCK * 4)
        return (
            pltpu.make_async_copy(k_hbm.at[rows], k_raw.at[rows], kl.at[b]),
            pltpu.make_async_copy(v_hbm.at[rows], v_raw.at[rows], vl.at[b]),
        )

    load_q.start()
    for b in range(BLOCKS):
        for copy in load_kv(b):
            copy.start()

    peers = [partner]
    for d in (1, 2, 3):
        for core in (0, 1):
            peers.append(dev(z, ahead(y, d), core))
            peers.append(dev(ahead(z, d), y, core))
        peers.append((seq, ahead(head, d)))
    barrier = pltpu.get_barrier_semaphore()
    for peer in peers:
        pl.semaphore_signal(barrier, inc=1, device_id=peer, device_id_type=MESH)

    load_q.wait()
    wide[0 : ROWS * 8, :] = q_raw[...].astype(f32)
    for h in range(8):
        qs[h] = wide[pl.ds(h, ROWS, stride=8), :].astype(bf16)
    qg[z, y, c] = qs[pl.ds(4 * c, 4)]

    length = len_ref[0]

    def prepare(b, _):
        for copy in load_kv(b):
            copy.wait()
        k0 = k_raw[0:8, :].astype(f32)
        rows = pl.ds(pl.multiple_of(b * BLOCK * 4, BLOCK * 4), BLOCK * 4)
        slots = pl.ds(pl.multiple_of(b * BLOCK, BLOCK), BLOCK)
        filled = lax.broadcasted_iota(jnp.int32, (BLOCK, HD), 0) + b * BLOCK < length
        wide[...] = k_raw[rows, :].astype(f32)
        for h in range(4):
            one = wide[pl.ds(h, BLOCK, stride=4), :]
            ks[h, slots, :] = jnp.where(filled, one, k0[h : h + 1, :]).astype(bf16)
        wide[...] = v_raw[rows, :].astype(f32)
        col = lax.broadcasted_iota(jnp.int32, (VROWS - HD, BLOCK), 1) + b * BLOCK
        row = lax.broadcasted_iota(jnp.int32, (VROWS - HD, BLOCK), 0)
        ones = jnp.where((col < length) & (row == 0), 1.0, 0.0).astype(bf16)
        for h in range(4):
            one = wide[pl.ds(h, BLOCK, stride=4), :]
            one = jnp.where(filled, one, 0.0).T.astype(bf16)
            for e in range(BLOCK // HD):
                lanes = slice(e * HD, (e + 1) * HD)
                vs[h, b * (BLOCK // HD) + e, 0:HD, :] = one[:, lanes]
                vs[h, b * (BLOCK // HD) + e, HD:VROWS, :] = ones[:, lanes]
        return 0

    def swap_kv(b):
        slots = pl.ds(pl.multiple_of(b * BLOCK, BLOCK), BLOCK)
        parts = pl.ds(b * (BLOCK // HD), BLOCK // HD)
        return (
            remote(ks.at[pl.ds(2 * p, 2), slots], kp.at[:, slots], ksend.at[b], krecv.at[b], partner),
            remote(
                vs.at[pl.ds(2 * p, 2), parts], vp.at[:, parts], vsend.at[b], vrecv.at[b], partner
            ),
        )

    lax.fori_loop(0, 2, prepare, 0)
    pl.semaphore_wait(barrier, len(peers))

    first = [remote(qs.at[pl.ds(4 * p, 4)], qg.at[z, y, c], psend, precv, partner)]
    for d in (1, 3, 2):
        for core in (0, 1):
            first.append(
                remote(
                    qs.at[pl.ds(4 * core, 2)], qg.at[z, y, c, pl.ds(0, 2)],
                    ysend.at[d - 1, core], yrecv.at[d - 1, c], dev(z, ahead(y, d), core),
                )
            )
            first.append(
                remote(
                    qs.at[pl.ds(4 * core + 2, 2)], qg.at[z, y, c, pl.ds(2, 2)],
                    zsend.at[d - 1, core], zrecv.at[d - 1, c], dev(ahead(z, d), y, core),
                )
            )

    @pl.when(c == 0)
    def _():
        for copy in first:
            copy.start()

    for b in (0, 1):
        for copy in swap_kv(b):
            copy.start()

    def prepare_and_swap(b, _):
        prepare(b, 0)

        @pl.when(b > 2)
        def _():
            for copy in swap_kv(b - 1):
                copy.start()

        return 0

    lax.fori_loop(2, BLOCKS, prepare_and_swap, 0)

    @pl.when(c == 1)
    def _():
        for copy in first:
            copy.start()

    for copy in swap_kv(BLOCKS - 1):
        copy.start()
    load_w.start()

    last_chip = (z == 3) & (y == 3)
    offset = off_ref[0] - 30 * SLOTS

    def chips(group, d, j):
        if group == 0:
            return [(ahead(z, d), ahead(y, 2 * j + e)) for e in (0, 1)]
        return [(ahead(z, 2 * j + e), ahead(y, d)) for e in (0, 1)]

    def queries_of(group, w, d, j):
        parts = [qg[zq, yq, w, group * 2 + h] for zq, yq in chips(group, d, j) for h in (0, 1)]
        q = jnp.concatenate(parts, axis=0).astype(f32) * score_scale
        high = q.astype(bf16)
        low = (q - high.astype(f32)).astype(bf16)
        return jnp.concatenate([high, low], axis=1)

    def limit_of(group, w, d, j):
        lane = lax.broadcasted_iota(jnp.int32, (8, 256), 1)
        (za, ya), (zb, yb) = chips(group, d, j)
        chip = jnp.where(lane < HD, za * 4 + ya, zb * 4 + yb)
        row = chip * HD + w * ROWS + lane % ROWS
        return offset + row - lax.broadcasted_iota(jnp.int32, (8, 256), 0)

    def scores(qq, limit, group, shard, s_ref, m):
        k = ks[2 * c + group] if shard == 0 else kp[group]
        kk = jnp.concatenate([k, k], axis=1)
        s = lax.dot_general(kk, qq, (((1,), (1,)), ((), ())), preferred_element_type=f32)
        s = s.reshape(SLOTS // 8, 8, 256)
        if limit is not None:
            room = limit - SLOTS * (c if shard == 0 else p)
            s = jnp.stack(
                [jnp.where(room >= 8 * i, s[i], masked_score) for i in range(SLOTS // 8)]
            )
        s_ref[pl.ds(shard * SLOTS, SLOTS), :] = s.reshape(SLOTS, 256)
        return jnp.maximum(m, jnp.max(s, axis=0))

    def weigh(s_ref, m_now, group, shard, acc):
        s = s_ref[pl.ds(shard * SLOTS, SLOTS), :].reshape(SLOTS // 8, 8, 256)
        prob = jnp.exp2(s - m_now[None]).reshape(SLOTS, 256).astype(bf16)
        parts = [
            vs[2 * c + group, e] if shard == 0 else vp[group, e] for e in range(SLOTS // HD)
        ]
        return acc + jnp.dot(jnp.concatenate(parts, axis=1), prob, preferred_element_type=f32)

    score_refs = ((sa0, sa1), (sb0, sb1))

    def tiles(new, cur, side, causal):
        for group in (0, 1):
            m = jnp.full((8, 256), masked_score, f32)
            if new is not None:
                qq = queries_of(group, *new)
                limit = limit_of(group, *new) if causal else None
            if cur is not None:
                m_now = tops[side, group]
            acc = jnp.zeros((VROWS, 256), f32)
            for shard in (0, 1):
                if new is not None:
                    m = scores(qq, limit, group, shard, score_refs[1 - side][group], m)
                if cur is not None:
                    acc = weigh(score_refs[side][group], m_now, group, shard, acc)
            if cur is not None:
                w, d, j = cur
                o_own[group, w, d, j] = acc[:HD].astype(bf16)
                m_own[group, w, d, j, 0:1, :] = m_now[0:1]
                m_own[group, w, d, j, 1:2, :] = acc[HD : HD + 1]
            if new is not None:
                tops[1 - side, group] = jnp.broadcast_to(
                    jnp.max(m, axis=0, keepdims=True), (8, 256)
                )

    def both(new, cur, side, when=True):
        @pl.when(jnp.logical_not(last_chip) & when)
        def _():
            tiles(new, cur, side, False)

        @pl.when(last_chip & when)
        def _():
            tiles(new, cur, side, True)

    def step(u):
        w = u // 8
        k = lax.rem(lax.rem(u, 8) // 2 + w, 4)
        return w, lax.rem(k * (k + 1) // 2, 4), lax.rem(u, 2)

    def sends(group, w, d, j):
        target = dev(ahead(z, d), y, c) if group == 0 else dev(z, ahead(y, d), c)
        slot = (group, w, d - 1, j)
        return (
            remote(m_own.at[group, w, d, j], inm1.at[slot], s1ms.at[slot], s1mr.at[slot], target),
            remote(o_own.at[group, w, d, j], in1.at[slot], s1s.at[slot], s1r.at[slot], target),
        )

    def send_tile(group, u):
        w, d, j = step(u)

        @pl.when(d > 0)
        def _():
            for copy in sends(group, w, d, j):
                copy.start()

    def passes(group, w, i):
        if i == 0:
            target = partner
        else:
            target = dev(z, ahead(y, i), w) if group == 0 else dev(ahead(z, i), y, w)
        return (
            remote(
                midm.at[group, w, i], inm2.at[c, group, i],
                s2ms.at[group, w, i], s2mr.at[c, group, i], target,
            ),
            remote(
                mid.at[group, w, i], in2.at[c, group, i],
                s2s.at[group, w, i], s2r.at[c, group, i], target,
            ),
        )

    def sum_first(group, w, j):
        for d in (1, 2, 3):
            for copy in sends(group, w, d, j):
                copy.wait_recv()
        parts = [
            (o_own[group, w, 0, j], m_own[group, w, 0, j, 0:1, :], m_own[group, w, 0, j, 1:2, :])
        ]
        for d in range(3):
            parts.append(
                (in1[group, w, d, j], inm1[group, w, d, j, 0:1, :], inm1[group, w, d, j, 1:2, :])
            )
        numer, top, denom = merge(parts)
        for e in (0, 1):
            i = 2 * j + e
            lanes = slice(e * HD, (e + 1) * HD)
            mid[group, w, i] = numer[:, lanes].astype(bf16)
            midm[group, w, i, 0:1, :] = top[:, lanes]
            midm[group, w, i, 1:2, :] = denom[:, lanes]
        for e in (1, 0):
            i = 2 * j + e
            if i:
                for copy in passes(group, w, i):
                    copy.start()
            else:

                @pl.when(c != w)
                def _():
                    for copy in passes(group, w, 0):
                        copy.start()

                @pl.when(c == w)
                def _():
                    in2[c, group, 0] = mid[group, w, 0]
                    inm2[c, group, 0] = midm[group, w, 0]

    def exchange(d):
        return remote(
            part.at[d - 1], inx.at[d - 1], xs.at[d - 1], xr.at[d - 1], (seq, ahead(head, d))
        )

    def project(w):
        for group in (0, 1):
            for source in (0, 1):
                for i in range(4):
                    if i or source != w:
                        slot = (source, group, i)
                        remote(
                            midm.at[group, w, i], inm2.at[slot],
                            s2ms.at[group, w, i], s2mr.at[slot], partner,
                        ).wait_recv()
                        remote(
                            mid.at[group, w, i], in2.at[slot],
                            s2s.at[group, w, i], s2r.at[slot], partner,
                        ).wait_recv()
        for source in (0, 1):
            for group in (0, 1):
                parts = [
                    (
                        in2[source, group, i],
                        inm2[source, group, i, 0:1, :],
                        inm2[source, group, i, 1:2, :],
                    )
                    for i in range(4)
                ]
                numer, _, denom = merge(parts)
                rows = (numer / denom).T.astype(bf16)
                first_col = (source * 2 + group) * 2 * HD
                for h in (0, 1):
                    cols = slice(first_col + h * HD, first_col + (h + 1) * HD)
                    lhs[:, cols] = rows[h * ROWS : (h + 1) * ROWS]
        load_w.wait()
        left = lhs[...]
        for d in (2, 1, 3, 0):
            cols = pl.ds(pl.multiple_of(ahead(head, d) * COLS, HD), COLS)
            block = jnp.dot(left, w_vmem[:, cols], preferred_element_type=f32)
            if d:
                part[d - 1] = block.astype(bf16)
                exchange(d).start()
            else:
                total[...] = block

    def finish():
        for d in (1, 2, 3):
            exchange(d).wait()
        out_ref[...] = total[...] + (
            (inx[0].astype(f32) + inx[1].astype(f32)) + inx[2].astype(f32)
        )

    def wait_first(core):
        @pl.when(c != core)
        def _():
            first[0].wait_recv()

        for d in (1, 2, 3):
            remote(
                qs.at[pl.ds(0, 2)], qg.at[z, ahead(y, 4 - d), core, pl.ds(0, 2)],
                ysend.at[d - 1, core], yrecv.at[d - 1, core], partner,
            ).wait_recv()
            remote(
                qs.at[pl.ds(0, 2)], qg.at[ahead(z, 4 - d), y, core, pl.ds(2, 2)],
                zsend.at[d - 1, core], zrecv.at[d - 1, core], partner,
            ).wait_recv()

    wait_first(0)

    def forward(group, w, d, back):
        if group == 0:
            src = qg.at[ahead(z, d) if back else z, :, w, pl.ds(0, 2)]
            target = dev(ahead(z, 4 - d), y, c)
        else:
            src = qg.at[:, ahead(y, d) if back else y, w, pl.ds(2, 2)]
            target = dev(z, ahead(y, 4 - d), c)
        slot = (group, w, d - 1)
        return remote(src, src, fsend.at[slot], frecv.at[slot], target)

    second = {(w, d): [forward(g, w, d, False) for g in (0, 1)] for w in (0, 1) for d in (1, 3, 2)}

    def start_forward(w, *ds):
        for d in ds:
            for copy in second[w, d]:
                copy.start()

    start_forward(0, 1, 3)

    def wait_swap(b, _):
        for copy in swap_kv(b):
            copy.wait()
        return 0

    lax.fori_loop(0, BLOCKS, wait_swap, 0)
    both(step(0), None, 1)

    def after(u):
        send_tile(0, u)
        send_tile(1, u)

        @pl.when(u == 0)
        def _():
            start_forward(0, 2)

        @pl.when(u == 2)
        def _():
            wait_first(1)
            start_forward(1, 1, 3)

        @pl.when(u == 4)
        def _():
            start_forward(1, 2)

        w, d, j = step(u + 2)

        @pl.when((j == 0) & (d > 0) & (u < 14))
        def _():
            for group in (0, 1):
                forward(group, w, d, True).wait_recv()

        @pl.when(u == 9)
        def _():
            for j in (0, 1):
                for group in (0, 1):
                    sum_first(group, 0, j)

        @pl.when((u == 11) & (c == 0))
        def _():
            project(0)

        @pl.when(u == 14)
        def _():
            for group in (0, 1):
                sum_first(group, 1, 0)

    def body(v, _):
        u = 2 * v
        both(step(u + 1), step(u), 0)
        after(u)
        both(step(u + 2), step(u + 1), 1, u < 14)

        @pl.when(u < 14)
        def _():
            after(u + 1)

        return 0

    lax.fori_loop(0, 8, body, 0)
    both(None, step(15), 1)
    for group in (0, 1):
        sum_first(group, 1, 1)

    @pl.when(c == 1)
    def _():
        project(1)

    for copy in first:
        copy.wait_send()
    for copies in second.values():
        for copy in copies:
            copy.wait_send()
    for group in (0, 1):
        for w in (0, 1):
            for j in (0, 1):
                for d in (1, 2, 3):
                    for copy in sends(group, w, d, j):
                        copy.wait_send()
            for i in (1, 2, 3):
                for copy in passes(group, w, i):
                    copy.wait_send()

            @pl.when(c != w)
            def _():
                for copy in passes(group, w, 0):
                    copy.wait_send()

    finish()


def shards(queries, keys, values, kv_len, causal_offset, out_weight):
    dma = pltpu.SemaphoreType.DMA
    hbm = pl.BlockSpec(memory_space=pl.ANY)
    smem = pl.BlockSpec(memory_space=pltpu.SMEM)

    def vmem(*shape, dtype=bf16):
        return pltpu.VMEM(shape, dtype)

    return pl.pallas_call(
        kernel,
        out_shape=jax.ShapeDtypeStruct((ROWS, COLS), f32),
        in_specs=[smem, smem, hbm, hbm, hbm, hbm],
        out_specs=pl.BlockSpec(memory_space=pltpu.VMEM),
        scratch_shapes=[
            vmem(ROWS * 8, HD),
            vmem(SLOTS * 4, HD),
            vmem(SLOTS * 4, HD),
            vmem(1024, 4608),
            vmem(BLOCK * 4, HD, dtype=f32),
            vmem(8, ROWS, HD),
            vmem(4, SLOTS, HD),
            vmem(4, SLOTS // HD, VROWS, HD),
            vmem(2, SLOTS, HD),
            vmem(2, SLOTS // HD, VROWS, HD),
            vmem(4, 4, 2, 4, ROWS, HD),
            vmem(2 * SLOTS, 256, dtype=f32),
            vmem(2 * SLOTS, 256, dtype=f32),
            vmem(2 * SLOTS, 256, dtype=f32),
            vmem(2 * SLOTS, 256, dtype=f32),
            vmem(2, 2, 8, 256, dtype=f32),
            vmem(2, 2, 4, 2, HD, 256),
            vmem(2, 2, 4, 2, 2, 256, dtype=f32),
            vmem(2, 2, 3, 2, HD, 256),
            vmem(2, 2, 3, 2, 2, 256, dtype=f32),
            vmem(2, 2, 4, HD, HD),
            vmem(2, 2, 4, 2, HD, dtype=f32),
            vmem(2, 2, 4, HD, HD),
            vmem(2, 2, 4, 2, HD, dtype=f32),
            vmem(ROWS, 1024),
            vmem(3, ROWS, COLS),
            vmem(ROWS, COLS, dtype=f32),
            vmem(3, ROWS, COLS),
            dma((2,)), dma((BLOCKS,)), dma((BLOCKS,)),
            dma, dma,
            dma((3, 2)), dma((3, 2)), dma((3, 2)), dma((3, 2)),
            dma((2, 2, 3)), dma((2, 2, 3)),
            dma((BLOCKS,)), dma((BLOCKS,)), dma((BLOCKS,)), dma((BLOCKS,)),
            dma((2, 2, 3, 2)), dma((2, 2, 3, 2)), dma((2, 2, 3, 2)), dma((2, 2, 3, 2)),
            dma((2, 2, 4)), dma((2, 2, 4)), dma((2, 2, 4)), dma((2, 2, 4)),
            dma((3,)), dma((3,)),
        ],
        compiler_params=pltpu.CompilerParams(
            collective_id=0, has_side_effects=True, vmem_limit_bytes=60 * 2**20
        ),
        name="attend",
    )(
        kv_len,
        causal_offset,
        queries.reshape(ROWS * 8, HD),
        keys.reshape(SLOTS * 4, HD),
        values.reshape(SLOTS * 4, HD),
        out_weight,
    )


def solution(mesh):
    placed = (
        P("seq", "head", None),
        P("seq", "head", None),
        P("seq", "head", None),
        P("seq"),
        P(),
        P("head", None),
    )
    return jax.shard_map(
        shards, mesh=mesh, in_specs=placed, out_specs=P("seq", "head"), check_vma=False
    )
```

```python
import math

import jax
import jax.numpy as jnp
from jax import lax
from jax.experimental import pallas as pl
from jax.experimental.pallas import tpu as pltpu
from jax.sharding import PartitionSpec as P

bf16 = jnp.bfloat16
f32 = jnp.float32
MESH = pl.DeviceIdType.MESH
score_scale = math.log2(math.e) / 12.0
masked_score = -1e30
HD = 128
ROWS = 64
SLOTS = 2048
VROWS = 144
COLS = 1152
BLOCK = 256
BLOCKS = SLOTS // BLOCK


def remote(src, dst, send_sem, recv_sem, device):
    return pltpu.make_async_remote_copy(
        src_ref=src,
        dst_ref=dst,
        send_sem=send_sem,
        recv_sem=recv_sem,
        device_id=device,
        device_id_type=MESH,
    )


def merge(parts):
    top = parts[0][1]
    for _, m, _ in parts[1:]:
        top = jnp.maximum(top, m)
    numer, denom = None, None
    for o, m, l in parts:
        factor = jnp.exp2(m - top)
        o = o.astype(f32) * factor
        l = l * factor
        numer = o if numer is None else numer + o
        denom = l if denom is None else denom + l
    return numer, top, denom


def kernel(
    len_ref, off_ref, q_hbm, k_hbm, v_hbm, w_hbm, out_ref,
    q_raw, k_raw, v_raw, w_vmem, wide, qs, ks, vs, kp, vp, qg, sa0, sa1, sb0, sb1, tops,
    o_own, m_own, in1, inm1, mid, midm, in2, inm2, lhs, part, total, inx,
    lsem, kl, vl, psend, precv, ysend, yrecv, zsend, zrecv, fsend, frecv,
    ksend, krecv, vsend, vrecv, s1s, s1r, s1ms, s1mr, s2s, s2r, s2ms, s2mr, xs, xr,
):
    seq = lax.axis_index("seq")
    head = lax.axis_index("head")
    z, y, c = seq // 8, (seq // 2) % 4, seq % 2
    p = 1 - c

    def dev(zt, yt, core):
        return ((zt * 4 + yt) * 2 + core, head)

    def ahead(index, d):
        return lax.rem(index + d, 4)

    partner = dev(z, y, p)

    load_q = pltpu.make_async_copy(q_hbm, q_raw, lsem.at[0])
    load_w = pltpu.make_async_copy(w_hbm, w_vmem, lsem.at[1])

    def load_kv(b):
        rows = pl.ds(pl.multiple_of(b * BLOCK * 4, BLOCK * 4), BLOCK * 4)
        return (
            pltpu.make_async_copy(k_hbm.at[rows], k_raw.at[rows], kl.at[b]),
            pltpu.make_async_copy(v_hbm.at[rows], v_raw.at[rows], vl.at[b]),
        )

    load_q.start()
    for b in range(BLOCKS):
        for copy in load_kv(b):
            copy.start()

    peers = [partner]
    for d in (1, 2, 3):
        for core in (0, 1):
            peers.append(dev(z, ahead(y, d), core))
            peers.append(dev(ahead(z, d), y, core))
        peers.append((seq, ahead(head, d)))
    barrier = pltpu.get_barrier_semaphore()
    for peer in peers:
        pl.semaphore_signal(barrier, inc=1, device_id=peer, device_id_type=MESH)

    load_q.wait()
    wide[0 : ROWS * 8, :] = q_raw[...].astype(f32)
    for h in range(8):
        qs[h] = wide[pl.ds(h, ROWS, stride=8), :].astype(bf16)
    qg[z, y, c] = qs[pl.ds(4 * c, 4)]

    length = len_ref[0]

    def prepare(b, _):
        for copy in load_kv(b):
            copy.wait()
        k0 = k_raw[0:8, :].astype(f32)
        rows = pl.ds(pl.multiple_of(b * BLOCK * 4, BLOCK * 4), BLOCK * 4)
        slots = pl.ds(pl.multiple_of(b * BLOCK, BLOCK), BLOCK)
        filled = lax.broadcasted_iota(jnp.int32, (BLOCK, HD), 0) + b * BLOCK < length
        wide[...] = k_raw[rows, :].astype(f32)
        for h in range(4):
            one = wide[pl.ds(h, BLOCK, stride=4), :]
            ks[h, slots, :] = jnp.where(filled, one, k0[h : h + 1, :]).astype(bf16)
        wide[...] = v_raw[rows, :].astype(f32)
        col = lax.broadcasted_iota(jnp.int32, (VROWS - HD, BLOCK), 1) + b * BLOCK
        row = lax.broadcasted_iota(jnp.int32, (VROWS - HD, BLOCK), 0)
        ones = jnp.where((col < length) & (row == 0), 1.0, 0.0).astype(bf16)
        for h in range(4):
            one = wide[pl.ds(h, BLOCK, stride=4), :]
            one = jnp.where(filled, one, 0.0).T.astype(bf16)
            for e in range(BLOCK // HD):
                lanes = slice(e * HD, (e + 1) * HD)
                vs[h, b * (BLOCK // HD) + e, 0:HD, :] = one[:, lanes]
                vs[h, b * (BLOCK // HD) + e, HD:VROWS, :] = ones[:, lanes]
        return 0

    def swap_kv(b):
        slots = pl.ds(pl.multiple_of(b * BLOCK, BLOCK), BLOCK)
        parts = pl.ds(b * (BLOCK // HD), BLOCK // HD)
        return (
            remote(ks.at[pl.ds(2 * p, 2), slots], kp.at[:, slots], ksend.at[b], krecv.at[b], partner),
            remote(
                vs.at[pl.ds(2 * p, 2), parts], vp.at[:, parts], vsend.at[b], vrecv.at[b], partner
            ),
        )

    pl.semaphore_wait(barrier, len(peers))

    first = [remote(qs.at[pl.ds(4 * p, 4)], qg.at[z, y, c], psend, precv, partner)]
    for d in (1, 3, 2):
        for core in (0, 1):
            first.append(
                remote(
                    qs.at[pl.ds(4 * core, 2)], qg.at[z, y, c, pl.ds(0, 2)],
                    ysend.at[d - 1, core], yrecv.at[d - 1, c], dev(z, ahead(y, d), core),
                )
            )
            first.append(
                remote(
                    qs.at[pl.ds(4 * core + 2, 2)], qg.at[z, y, c, pl.ds(2, 2)],
                    zsend.at[d - 1, core], zrecv.at[d - 1, c], dev(ahead(z, d), y, core),
                )
            )

    @pl.when(c == 0)
    def _():
        for copy in first:
            copy.start()

    def prepare_and_swap(b, _):
        prepare(b, 0)

        @pl.when(b > 0)
        def _():
            for copy in swap_kv(b - 1):
                copy.start()

        return 0

    lax.fori_loop(0, BLOCKS, prepare_and_swap, 0)

    @pl.when(c == 1)
    def _():
        for copy in first:
            copy.start()

    for copy in swap_kv(BLOCKS - 1):
        copy.start()
    load_w.start()

    last_chip = (z == 3) & (y == 3)
    offset = off_ref[0] - 30 * SLOTS

    def chips(group, d, j):
        if group == 0:
            return [(ahead(z, d), ahead(y, 2 * j + e)) for e in (0, 1)]
        return [(ahead(z, 2 * j + e), ahead(y, d)) for e in (0, 1)]

    def queries_of(group, w, d, j):
        parts = [qg[zq, yq, w, group * 2 + h] for zq, yq in chips(group, d, j) for h in (0, 1)]
        q = jnp.concatenate(parts, axis=0).astype(f32) * score_scale
        high = q.astype(bf16)
        low = (q - high.astype(f32)).astype(bf16)
        return jnp.concatenate([high, low], axis=1)

    def limit_of(group, w, d, j):
        lane = lax.broadcasted_iota(jnp.int32, (8, 256), 1)
        (za, ya), (zb, yb) = chips(group, d, j)
        chip = jnp.where(lane < HD, za * 4 + ya, zb * 4 + yb)
        row = chip * HD + w * ROWS + lane % ROWS
        return offset + row - lax.broadcasted_iota(jnp.int32, (8, 256), 0)

    def scores(qq, limit, group, shard, s_ref, m):
        k = ks[2 * c + group] if shard == 0 else kp[group]
        kk = jnp.concatenate([k, k], axis=1)
        s = lax.dot_general(kk, qq, (((1,), (1,)), ((), ())), preferred_element_type=f32)
        s = s.reshape(SLOTS // 8, 8, 256)
        if limit is not None:
            room = limit - SLOTS * (c if shard == 0 else p)
            s = jnp.stack(
                [jnp.where(room >= 8 * i, s[i], masked_score) for i in range(SLOTS // 8)]
            )
        s_ref[pl.ds(shard * SLOTS, SLOTS), :] = s.reshape(SLOTS, 256)
        return jnp.maximum(m, jnp.max(s, axis=0))

    def weigh(s_ref, m_now, group, shard, acc):
        s = s_ref[pl.ds(shard * SLOTS, SLOTS), :].reshape(SLOTS // 8, 8, 256)
        prob = jnp.exp2(s - m_now[None]).reshape(SLOTS, 256).astype(bf16)
        parts = [
            vs[2 * c + group, e] if shard == 0 else vp[group, e] for e in range(SLOTS // HD)
        ]
        return acc + jnp.dot(jnp.concatenate(parts, axis=1), prob, preferred_element_type=f32)

    score_refs = ((sa0, sa1), (sb0, sb1))

    def tiles(new, cur, side, causal):
        for group in (0, 1):
            m = jnp.full((8, 256), masked_score, f32)
            if new is not None:
                qq = queries_of(group, *new)
                limit = limit_of(group, *new) if causal else None
            if cur is not None:
                m_now = tops[side, group]
            acc = jnp.zeros((VROWS, 256), f32)
            for shard in (0, 1):
                if new is not None:
                    m = scores(qq, limit, group, shard, score_refs[1 - side][group], m)
                if cur is not None:
                    acc = weigh(score_refs[side][group], m_now, group, shard, acc)
            if cur is not None:
                w, d, j = cur
                o_own[group, w, d, j] = acc[:HD].astype(bf16)
                m_own[group, w, d, j, 0:1, :] = m_now[0:1]
                m_own[group, w, d, j, 1:2, :] = acc[HD : HD + 1]
            if new is not None:
                tops[1 - side, group] = jnp.broadcast_to(
                    jnp.max(m, axis=0, keepdims=True), (8, 256)
                )

    def both(new, cur, side, when=True):
        @pl.when(jnp.logical_not(last_chip) & when)
        def _():
            tiles(new, cur, side, False)

        @pl.when(last_chip & when)
        def _():
            tiles(new, cur, side, True)

    def step(u):
        w = u // 8
        k = lax.rem(u, 8) // 2
        d = (1 - w) * lax.rem(k * (k + 1) // 2, 4) + w * (3 - k)
        return w, d, lax.rem(u, 2)

    def sends(group, w, d, j):
        target = dev(ahead(z, d), y, c) if group == 0 else dev(z, ahead(y, d), c)
        slot = (group, w, d - 1, j)
        return (
            remote(m_own.at[group, w, d, j], inm1.at[slot], s1ms.at[slot], s1mr.at[slot], target),
            remote(o_own.at[group, w, d, j], in1.at[slot], s1s.at[slot], s1r.at[slot], target),
        )

    def send_tile(group, u):
        w, d, j = step(u)

        @pl.when(d > 0)
        def _():
            for copy in sends(group, w, d, j):
                copy.start()

    def passes(group, w, i):
        if i == 0:
            target = partner
        else:
            target = dev(z, ahead(y, i), w) if group == 0 else dev(ahead(z, i), y, w)
        return (
            remote(
                midm.at[group, w, i], inm2.at[c, group, i],
                s2ms.at[group, w, i], s2mr.at[c, group, i], target,
            ),
            remote(
                mid.at[group, w, i], in2.at[c, group, i],
                s2s.at[group, w, i], s2r.at[c, group, i], target,
            ),
        )

    def sum_first(group, w, j):
        for d in (1, 2, 3):
            for copy in sends(group, w, d, j):
                copy.wait_recv()
        parts = [
            (o_own[group, w, 0, j], m_own[group, w, 0, j, 0:1, :], m_own[group, w, 0, j, 1:2, :])
        ]
        for d in range(3):
            parts.append(
                (in1[group, w, d, j], inm1[group, w, d, j, 0:1, :], inm1[group, w, d, j, 1:2, :])
            )
        numer, top, denom = merge(parts)
        for e in (0, 1):
            i = 2 * j + e
            lanes = slice(e * HD, (e + 1) * HD)
            mid[group, w, i] = numer[:, lanes].astype(bf16)
            midm[group, w, i, 0:1, :] = top[:, lanes]
            midm[group, w, i, 1:2, :] = denom[:, lanes]
        for e in (1, 0):
            i = 2 * j + e
            if i:
                for copy in passes(group, w, i):
                    copy.start()
            else:

                @pl.when(c != w)
                def _():
                    for copy in passes(group, w, 0):
                        copy.start()

                @pl.when(c == w)
                def _():
                    in2[c, group, 0] = mid[group, w, 0]
                    inm2[c, group, 0] = midm[group, w, 0]

    def exchange(d):
        return remote(
            part.at[d - 1], inx.at[d - 1], xs.at[d - 1], xr.at[d - 1], (seq, ahead(head, d))
        )

    def project(w):
        for group in (0, 1):
            for source in (0, 1):
                for i in range(4):
                    if i or source != w:
                        slot = (source, group, i)
                        remote(
                            midm.at[group, w, i], inm2.at[slot],
                            s2ms.at[group, w, i], s2mr.at[slot], partner,
                        ).wait_recv()
                        remote(
                            mid.at[group, w, i], in2.at[slot],
                            s2s.at[group, w, i], s2r.at[slot], partner,
                        ).wait_recv()
        for source in (0, 1):
            for group in (0, 1):
                parts = [
                    (
                        in2[source, group, i],
                        inm2[source, group, i, 0:1, :],
                        inm2[source, group, i, 1:2, :],
                    )
                    for i in range(4)
                ]
                numer, _, denom = merge(parts)
                rows = (numer / denom).T.astype(bf16)
                first_col = (source * 2 + group) * 2 * HD
                for h in (0, 1):
                    cols = slice(first_col + h * HD, first_col + (h + 1) * HD)
                    lhs[:, cols] = rows[h * ROWS : (h + 1) * ROWS]
        load_w.wait()
        left = lhs[...]
        for d in (2, 1, 3, 0):
            cols = pl.ds(pl.multiple_of(ahead(head, d) * COLS, HD), COLS)
            block = jnp.dot(left, w_vmem[:, cols], preferred_element_type=f32)
            if d:
                part[d - 1] = block.astype(bf16)
                exchange(d).start()
            else:
                total[...] = block

    def finish():
        for d in (1, 2, 3):
            exchange(d).wait()
        out_ref[...] = total[...] + (
            (inx[0].astype(f32) + inx[1].astype(f32)) + inx[2].astype(f32)
        )

    def wait_first(core):
        @pl.when(c != core)
        def _():
            first[0].wait_recv()

        for d in (1, 2, 3):
            remote(
                qs.at[pl.ds(0, 2)], qg.at[z, ahead(y, 4 - d), core, pl.ds(0, 2)],
                ysend.at[d - 1, core], yrecv.at[d - 1, core], partner,
            ).wait_recv()
            remote(
                qs.at[pl.ds(0, 2)], qg.at[ahead(z, 4 - d), y, core, pl.ds(2, 2)],
                zsend.at[d - 1, core], zrecv.at[d - 1, core], partner,
            ).wait_recv()

    wait_first(0)

    def forward(group, w, d, back):
        if group == 0:
            src = qg.at[ahead(z, d) if back else z, :, w, pl.ds(0, 2)]
            target = dev(ahead(z, 4 - d), y, c)
        else:
            src = qg.at[:, ahead(y, d) if back else y, w, pl.ds(2, 2)]
            target = dev(z, ahead(y, 4 - d), c)
        slot = (group, w, d - 1)
        return remote(src, src, fsend.at[slot], frecv.at[slot], target)

    second = {(w, d): [forward(g, w, d, False) for g in (0, 1)] for w in (0, 1) for d in (1, 3, 2)}

    def start_forward(w, *ds):
        for d in ds:
            for copy in second[w, d]:
                copy.start()

    start_forward(0, 1, 3)

    def wait_swap(b, _):
        for copy in swap_kv(b):
            copy.wait()
        return 0

    def open_with(shard, causal):
        for group in (0, 1):
            qq = queries_of(group, *step(0))
            limit = limit_of(group, *step(0)) if causal else None
            m = tops[0, group] if shard else jnp.full((8, 256), masked_score, f32)
            m = scores(qq, limit, group, shard, score_refs[0][group], m)
            tops[0, group] = jnp.broadcast_to(jnp.max(m, axis=0, keepdims=True), (8, 256))

    for shard in (0, 1):
        if shard:
            lax.fori_loop(0, BLOCKS, wait_swap, 0)

        @pl.when(jnp.logical_not(last_chip))
        def _():
            open_with(shard, False)

        @pl.when(last_chip)
        def _():
            open_with(shard, True)

    def after(u):
        send_tile(0, u)
        send_tile(1, u)

        @pl.when(u == 0)
        def _():
            start_forward(0, 2)

        @pl.when(u == 2)
        def _():
            wait_first(1)
            start_forward(1, 3, 2)

        @pl.when(u == 4)
        def _():
            start_forward(1, 1)

        w, d, j = step(u + 2)

        @pl.when((j == 0) & (d > 0) & (u < 14))
        def _():
            for group in (0, 1):
                forward(group, w, d, True).wait_recv()

        @pl.when(u == 9)
        def _():
            for j in (0, 1):
                for group in (0, 1):
                    sum_first(group, 0, j)

        @pl.when(u == 14)
        def _():
            for group in (0, 1):
                sum_first(group, 1, 0)

    def body(v, _):
        u = 2 * v
        both(step(u + 1), step(u), 0)
        after(u)
        both(step(u + 2), step(u + 1), 1, u < 14)

        @pl.when(u < 14)
        def _():
            after(u + 1)

        return 0

    lax.fori_loop(0, 8, body, 0)
    both(None, step(15), 1)
    for group in (0, 1):
        sum_first(group, 1, 1)

    @pl.when(c == 0)
    def _():
        project(0)

    @pl.when(c == 1)
    def _():
        project(1)

    for copy in first:
        copy.wait_send()
    for copies in second.values():
        for copy in copies:
            copy.wait_send()
    for group in (0, 1):
        for w in (0, 1):
            for j in (0, 1):
                for d in (1, 2, 3):
                    for copy in sends(group, w, d, j):
                        copy.wait_send()
            for i in (1, 2, 3):
                for copy in passes(group, w, i):
                    copy.wait_send()

            @pl.when(c != w)
            def _():
                for copy in passes(group, w, 0):
                    copy.wait_send()

    finish()


def shards(queries, keys, values, kv_len, causal_offset, out_weight):
    dma = pltpu.SemaphoreType.DMA
    hbm = pl.BlockSpec(memory_space=pl.ANY)
    smem = pl.BlockSpec(memory_space=pltpu.SMEM)

    def vmem(*shape, dtype=bf16):
        return pltpu.VMEM(shape, dtype)

    return pl.pallas_call(
        kernel,
        out_shape=jax.ShapeDtypeStruct((ROWS, COLS), f32),
        in_specs=[smem, smem, hbm, hbm, hbm, hbm],
        out_specs=pl.BlockSpec(memory_space=pltpu.VMEM),
        scratch_shapes=[
            vmem(ROWS * 8, HD),
            vmem(SLOTS * 4, HD),
            vmem(SLOTS * 4, HD),
            vmem(1024, 4608),
            vmem(BLOCK * 4, HD, dtype=f32),
            vmem(8, ROWS, HD),
            vmem(4, SLOTS, HD),
            vmem(4, SLOTS // HD, VROWS, HD),
            vmem(2, SLOTS, HD),
            vmem(2, SLOTS // HD, VROWS, HD),
            vmem(4, 4, 2, 4, ROWS, HD),
            vmem(2 * SLOTS, 256, dtype=f32),
            vmem(2 * SLOTS, 256, dtype=f32),
            vmem(2 * SLOTS, 256, dtype=f32),
            vmem(2 * SLOTS, 256, dtype=f32),
            vmem(2, 2, 8, 256, dtype=f32),
            vmem(2, 2, 4, 2, HD, 256),
            vmem(2, 2, 4, 2, 2, 256, dtype=f32),
            vmem(2, 2, 3, 2, HD, 256),
            vmem(2, 2, 3, 2, 2, 256, dtype=f32),
            vmem(2, 2, 4, HD, HD),
            vmem(2, 2, 4, 2, HD, dtype=f32),
            vmem(2, 2, 4, HD, HD),
            vmem(2, 2, 4, 2, HD, dtype=f32),
            vmem(ROWS, 1024),
            vmem(3, ROWS, COLS),
            vmem(ROWS, COLS, dtype=f32),
            vmem(3, ROWS, COLS),
            dma((2,)), dma((BLOCKS,)), dma((BLOCKS,)),
            dma, dma,
            dma((3, 2)), dma((3, 2)), dma((3, 2)), dma((3, 2)),
            dma((2, 2, 3)), dma((2, 2, 3)),
            dma((BLOCKS,)), dma((BLOCKS,)), dma((BLOCKS,)), dma((BLOCKS,)),
            dma((2, 2, 3, 2)), dma((2, 2, 3, 2)), dma((2, 2, 3, 2)), dma((2, 2, 3, 2)),
            dma((2, 2, 4)), dma((2, 2, 4)), dma((2, 2, 4)), dma((2, 2, 4)),
            dma((3,)), dma((3,)),
        ],
        compiler_params=pltpu.CompilerParams(
            collective_id=0, has_side_effects=True, vmem_limit_bytes=60 * 2**20
        ),
        name="attend",
    )(
        kv_len,
        causal_offset,
        queries.reshape(ROWS * 8, HD),
        keys.reshape(SLOTS * 4, HD),
        values.reshape(SLOTS * 4, HD),
        out_weight,
    )


def solution(mesh):
    placed = (
        P("seq", "head", None),
        P("seq", "head", None),
        P("seq", "head", None),
        P("seq"),
        P(),
        P("head", None),
    )
    return jax.shard_map(
        shards, mesh=mesh, in_specs=placed, out_specs=P("seq", "head"), check_vma=False
    )
```

```python
import math

import jax
import jax.numpy as jnp
from jax import lax
from jax.experimental import pallas as pl
from jax.experimental.pallas import tpu as pltpu
from jax.sharding import PartitionSpec as P

bf16 = jnp.bfloat16
f32 = jnp.float32
MESH = pl.DeviceIdType.MESH
score_scale = math.log2(math.e) / 12.0
masked_score = -1e30
HD = 128
ROWS = 64
SLOTS = 2048
VROWS = 144
COLS = 1152
BLOCK = 256
BLOCKS = SLOTS // BLOCK


def remote(src, dst, send_sem, recv_sem, device):
    return pltpu.make_async_remote_copy(
        src_ref=src,
        dst_ref=dst,
        send_sem=send_sem,
        recv_sem=recv_sem,
        device_id=device,
        device_id_type=MESH,
    )


def merge(parts):
    top = parts[0][1]
    for _, m, _ in parts[1:]:
        top = jnp.maximum(top, m)
    numer, denom = None, None
    for o, m, l in parts:
        factor = jnp.exp2(m - top)
        o = o.astype(f32) * factor
        l = l * factor
        numer = o if numer is None else numer + o
        denom = l if denom is None else denom + l
    return numer, top, denom


def kernel(
    len_ref, off_ref, q_hbm, k_hbm, v_hbm, w_hbm, out_ref,
    q_raw, k_raw, v_raw, w_vmem, wide, qs, ks, vs, kp, vp, qg, sa0, sa1, sb0, sb1, tops,
    o_own, m_own, in1, inm1, mid, midm, in2, inm2, lhs, part, total, inx,
    lsem, kl, vl, psend, precv, ysend, yrecv, zsend, zrecv, fsend, frecv,
    ksend, krecv, vsend, vrecv, s1s, s1r, s1ms, s1mr, s2s, s2r, s2ms, s2mr, xs, xr,
):
    seq = lax.axis_index("seq")
    head = lax.axis_index("head")
    z, y, c = seq // 8, (seq // 2) % 4, seq % 2
    p = 1 - c

    def dev(zt, yt, core):
        return ((zt * 4 + yt) * 2 + core, head)

    def ahead(index, d):
        return lax.rem(index + d, 4)

    partner = dev(z, y, p)

    load_q = pltpu.make_async_copy(q_hbm, q_raw, lsem.at[0])
    load_w = pltpu.make_async_copy(w_hbm, w_vmem, lsem.at[1])

    def load_kv(b):
        rows = pl.ds(pl.multiple_of(b * BLOCK * 4, BLOCK * 4), BLOCK * 4)
        return (
            pltpu.make_async_copy(k_hbm.at[rows], k_raw.at[rows], kl.at[b]),
            pltpu.make_async_copy(v_hbm.at[rows], v_raw.at[rows], vl.at[b]),
        )

    load_q.start()
    for b in range(BLOCKS):
        for copy in load_kv(b):
            copy.start()

    peers = [partner]
    for d in (1, 2, 3):
        for core in (0, 1):
            peers.append(dev(z, ahead(y, d), core))
            peers.append(dev(ahead(z, d), y, core))
        peers.append((seq, ahead(head, d)))
    barrier = pltpu.get_barrier_semaphore()
    for peer in peers:
        pl.semaphore_signal(barrier, inc=1, device_id=peer, device_id_type=MESH)

    load_q.wait()
    wide[0 : ROWS * 8, :] = q_raw[...].astype(f32)
    for h in range(8):
        qs[h] = wide[pl.ds(h, ROWS, stride=8), :].astype(bf16)
    qg[z, y, c] = qs[pl.ds(4 * c, 4)]

    length = len_ref[0]

    def prepare(b, _):
        for copy in load_kv(b):
            copy.wait()
        k0 = k_raw[0:8, :].astype(f32)
        rows = pl.ds(pl.multiple_of(b * BLOCK * 4, BLOCK * 4), BLOCK * 4)
        slots = pl.ds(pl.multiple_of(b * BLOCK, BLOCK), BLOCK)
        filled = lax.broadcasted_iota(jnp.int32, (BLOCK, HD), 0) + b * BLOCK < length
        wide[...] = k_raw[rows, :].astype(f32)
        for h in range(4):
            one = wide[pl.ds(h, BLOCK, stride=4), :]
            ks[h, slots, :] = jnp.where(filled, one, k0[h : h + 1, :]).astype(bf16)
        wide[...] = v_raw[rows, :].astype(f32)
        col = lax.broadcasted_iota(jnp.int32, (VROWS - HD, BLOCK), 1) + b * BLOCK
        row = lax.broadcasted_iota(jnp.int32, (VROWS - HD, BLOCK), 0)
        ones = jnp.where((col < length) & (row == 0), 1.0, 0.0).astype(bf16)
        for h in range(4):
            one = wide[pl.ds(h, BLOCK, stride=4), :]
            one = jnp.where(filled, one, 0.0).T.astype(bf16)
            for e in range(BLOCK // HD):
                lanes = slice(e * HD, (e + 1) * HD)
                vs[h, b * (BLOCK // HD) + e, 0:HD, :] = one[:, lanes]
                vs[h, b * (BLOCK // HD) + e, HD:VROWS, :] = ones[:, lanes]
        return 0

    def swap_kv(b):
        slots = pl.ds(pl.multiple_of(b * BLOCK, BLOCK), BLOCK)
        parts = pl.ds(b * (BLOCK // HD), BLOCK // HD)
        return (
            remote(ks.at[pl.ds(2 * p, 2), slots], kp.at[:, slots], ksend.at[b], krecv.at[b], partner),
            remote(
                vs.at[pl.ds(2 * p, 2), parts], vp.at[:, parts], vsend.at[b], vrecv.at[b], partner
            ),
        )

    pl.semaphore_wait(barrier, len(peers))

    first = [remote(qs.at[pl.ds(4 * p, 4)], qg.at[z, y, c], psend, precv, partner)]
    for d in (1, 3, 2):
        for core in (0, 1):
            first.append(
                remote(
                    qs.at[pl.ds(4 * core, 2)], qg.at[z, y, c, pl.ds(0, 2)],
                    ysend.at[d - 1, core], yrecv.at[d - 1, c], dev(z, ahead(y, d), core),
                )
            )
            first.append(
                remote(
                    qs.at[pl.ds(4 * core + 2, 2)], qg.at[z, y, c, pl.ds(2, 2)],
                    zsend.at[d - 1, core], zrecv.at[d - 1, c], dev(ahead(z, d), y, core),
                )
            )

    @pl.when(c == 0)
    def _():
        for copy in first:
            copy.start()

    def prepare_and_swap(b, _):
        prepare(b, 0)

        @pl.when(b > 0)
        def _():
            for copy in swap_kv(b - 1):
                copy.start()

        return 0

    lax.fori_loop(0, BLOCKS, prepare_and_swap, 0)

    @pl.when(c == 1)
    def _():
        for copy in first:
            copy.start()

    for copy in swap_kv(BLOCKS - 1):
        copy.start()
    load_w.start()

    last_chip = (z == 3) & (y == 3)
    offset = off_ref[0] - 30 * SLOTS

    def chips(group, d, j):
        if group == 0:
            return [(ahead(z, d), ahead(y, 2 * j + e)) for e in (0, 1)]
        return [(ahead(z, 2 * j + e), ahead(y, d)) for e in (0, 1)]

    def queries_of(group, w, d, j):
        parts = [qg[zq, yq, w, group * 2 + h] for zq, yq in chips(group, d, j) for h in (0, 1)]
        q = jnp.concatenate(parts, axis=0).astype(f32) * score_scale
        high = q.astype(bf16)
        low = (q - high.astype(f32)).astype(bf16)
        return jnp.concatenate([high, low], axis=1)

    def limit_of(group, w, d, j):
        lane = lax.broadcasted_iota(jnp.int32, (8, 256), 1)
        (za, ya), (zb, yb) = chips(group, d, j)
        chip = jnp.where(lane < HD, za * 4 + ya, zb * 4 + yb)
        row = chip * HD + w * ROWS + lane % ROWS
        return offset + row - lax.broadcasted_iota(jnp.int32, (8, 256), 0)

    def scores(qq, limit, group, shard, s_ref, m):
        k = ks[2 * c + group] if shard == 0 else kp[group]
        kk = jnp.concatenate([k, k], axis=1)
        s = lax.dot_general(kk, qq, (((1,), (1,)), ((), ())), preferred_element_type=f32)
        s = s.reshape(SLOTS // 8, 8, 256)
        if limit is not None:
            room = limit - SLOTS * (c if shard == 0 else p)
            s = jnp.stack(
                [jnp.where(room >= 8 * i, s[i], masked_score) for i in range(SLOTS // 8)]
            )
        s_ref[pl.ds(shard * SLOTS, SLOTS), :] = s.reshape(SLOTS, 256)
        return jnp.maximum(m, jnp.max(s, axis=0))

    def weigh(s_ref, m_now, group, shard, acc):
        s = s_ref[pl.ds(shard * SLOTS, SLOTS), :].reshape(SLOTS // 8, 8, 256)
        prob = jnp.exp2(s - m_now[None]).reshape(SLOTS, 256).astype(bf16)
        parts = [
            vs[2 * c + group, e] if shard == 0 else vp[group, e] for e in range(SLOTS // HD)
        ]
        return acc + jnp.dot(jnp.concatenate(parts, axis=1), prob, preferred_element_type=f32)

    score_refs = ((sa0, sa1), (sb0, sb1))

    def tiles(new, cur, side, causal):
        for group in (0, 1):
            m = jnp.full((8, 256), masked_score, f32)
            if new is not None:
                qq = queries_of(group, *new)
                limit = limit_of(group, *new) if causal else None
            if cur is not None:
                m_now = tops[side, group]
            acc = jnp.zeros((VROWS, 256), f32)
            for shard in (0, 1):
                if new is not None:
                    m = scores(qq, limit, group, shard, score_refs[1 - side][group], m)
                if cur is not None:
                    acc = weigh(score_refs[side][group], m_now, group, shard, acc)
            if cur is not None:
                w, d, j = cur
                o_own[group, w, d, j] = acc[:HD].astype(bf16)
                m_own[group, w, d, j, 0:1, :] = m_now[0:1]
                m_own[group, w, d, j, 1:2, :] = acc[HD : HD + 1]
            if new is not None:
                tops[1 - side, group] = jnp.broadcast_to(
                    jnp.max(m, axis=0, keepdims=True), (8, 256)
                )

    def both(new, cur, side, when=True):
        @pl.when(jnp.logical_not(last_chip) & when)
        def _():
            tiles(new, cur, side, False)

        @pl.when(last_chip & when)
        def _():
            tiles(new, cur, side, True)

    def step(u):
        w = u // 8
        k = lax.rem(u, 8) // 2
        k = lax.rem(k + w, 4)
        d = lax.rem(k * (k + 1) // 2, 4)
        return w, d, lax.rem(u, 2)

    def sends(group, w, d, j):
        target = dev(ahead(z, d), y, c) if group == 0 else dev(z, ahead(y, d), c)
        slot = (group, w, d - 1, j)
        return (
            remote(m_own.at[group, w, d, j], inm1.at[slot], s1ms.at[slot], s1mr.at[slot], target),
            remote(o_own.at[group, w, d, j], in1.at[slot], s1s.at[slot], s1r.at[slot], target),
        )

    def send_tile(group, u):
        w, d, j = step(u)

        @pl.when(d > 0)
        def _():
            for copy in sends(group, w, d, j):
                copy.start()

    def passes(group, w, i):
        if i == 0:
            target = partner
        else:
            target = dev(z, ahead(y, i), w) if group == 0 else dev(ahead(z, i), y, w)
        return (
            remote(
                midm.at[group, w, i], inm2.at[c, group, i],
                s2ms.at[group, w, i], s2mr.at[c, group, i], target,
            ),
            remote(
                mid.at[group, w, i], in2.at[c, group, i],
                s2s.at[group, w, i], s2r.at[c, group, i], target,
            ),
        )

    def sum_first(group, w, j):
        for d in (1, 2, 3):
            for copy in sends(group, w, d, j):
                copy.wait_recv()
        parts = [
            (o_own[group, w, 0, j], m_own[group, w, 0, j, 0:1, :], m_own[group, w, 0, j, 1:2, :])
        ]
        for d in range(3):
            parts.append(
                (in1[group, w, d, j], inm1[group, w, d, j, 0:1, :], inm1[group, w, d, j, 1:2, :])
            )
        numer, top, denom = merge(parts)
        for e in (0, 1):
            i = 2 * j + e
            lanes = slice(e * HD, (e + 1) * HD)
            mid[group, w, i] = numer[:, lanes].astype(bf16)
            midm[group, w, i, 0:1, :] = top[:, lanes]
            midm[group, w, i, 1:2, :] = denom[:, lanes]
        for e in (1, 0):
            i = 2 * j + e
            if i:
                for copy in passes(group, w, i):
                    copy.start()
            else:

                @pl.when(c != w)
                def _():
                    for copy in passes(group, w, 0):
                        copy.start()

                @pl.when(c == w)
                def _():
                    in2[c, group, 0] = mid[group, w, 0]
                    inm2[c, group, 0] = midm[group, w, 0]

    def exchange(d):
        return remote(
            part.at[d - 1], inx.at[d - 1], xs.at[d - 1], xr.at[d - 1], (seq, ahead(head, d))
        )

    def project(w):
        for group in (0, 1):
            for source in (0, 1):
                for i in range(4):
                    if i or source != w:
                        slot = (source, group, i)
                        remote(
                            midm.at[group, w, i], inm2.at[slot],
                            s2ms.at[group, w, i], s2mr.at[slot], partner,
                        ).wait_recv()
                        remote(
                            mid.at[group, w, i], in2.at[slot],
                            s2s.at[group, w, i], s2r.at[slot], partner,
                        ).wait_recv()
        for source in (0, 1):
            for group in (0, 1):
                parts = [
                    (
                        in2[source, group, i],
                        inm2[source, group, i, 0:1, :],
                        inm2[source, group, i, 1:2, :],
                    )
                    for i in range(4)
                ]
                numer, _, denom = merge(parts)
                rows = (numer / denom).T.astype(bf16)
                first_col = (source * 2 + group) * 2 * HD
                for h in (0, 1):
                    cols = slice(first_col + h * HD, first_col + (h + 1) * HD)
                    lhs[:, cols] = rows[h * ROWS : (h + 1) * ROWS]
        load_w.wait()
        left = lhs[...]
        for d in (2, 1, 3, 0):
            cols = pl.ds(pl.multiple_of(ahead(head, d) * COLS, HD), COLS)
            block = jnp.dot(left, w_vmem[:, cols], preferred_element_type=f32)
            if d:
                part[d - 1] = block.astype(bf16)
                exchange(d).start()
            else:
                total[...] = block

    def finish():
        for d in (1, 2, 3):
            exchange(d).wait()
        out_ref[...] = total[...] + (
            (inx[0].astype(f32) + inx[1].astype(f32)) + inx[2].astype(f32)
        )

    def wait_partner(core):
        @pl.when(c != core)
        def _():
            first[0].wait_recv()

    def wait_first(core):
        for d in (1, 2, 3):
            remote(
                qs.at[pl.ds(0, 2)], qg.at[z, ahead(y, 4 - d), core, pl.ds(0, 2)],
                ysend.at[d - 1, core], yrecv.at[d - 1, core], partner,
            ).wait_recv()
            remote(
                qs.at[pl.ds(0, 2)], qg.at[ahead(z, 4 - d), y, core, pl.ds(2, 2)],
                zsend.at[d - 1, core], zrecv.at[d - 1, core], partner,
            ).wait_recv()

    def forward(group, w, d, e, back):
        if group == 0:
            src = qg.at[ahead(z, d) if back else z, ahead(y, e), w, pl.ds(0, 2)]
            target = dev(ahead(z, 4 - d), y, c)
        else:
            src = qg.at[ahead(z, e), ahead(y, d) if back else y, w, pl.ds(2, 2)]
            target = dev(z, ahead(y, 4 - d), c)
        slot = (group, w, d - 1, e)
        return remote(src, src, fsend.at[slot], frecv.at[slot], target)

    def start_forward(w, ds, es):
        for e in es:
            for d in ds:
                for group in (0, 1):
                    forward(group, w, d, e, False).start()

    wait_partner(0)
    start_forward(0, (1, 3), (0,))
    wait_first(0)
    start_forward(0, (1, 3), (1, 2, 3))

    def wait_swap(b, _):
        for copy in swap_kv(b):
            copy.wait()
        return 0

    def open_with(shard, causal):
        for group in (0, 1):
            qq = queries_of(group, *step(0))
            limit = limit_of(group, *step(0)) if causal else None
            m = tops[0, group] if shard else jnp.full((8, 256), masked_score, f32)
            m = scores(qq, limit, group, shard, score_refs[0][group], m)
            tops[0, group] = jnp.broadcast_to(jnp.max(m, axis=0, keepdims=True), (8, 256))

    for shard in (0, 1):
        if shard:
            lax.fori_loop(0, BLOCKS, wait_swap, 0)

        @pl.when(jnp.logical_not(last_chip))
        def _():
            open_with(shard, False)

        @pl.when(last_chip)
        def _():
            open_with(shard, True)

    def after(u):
        send_tile(0, u)
        send_tile(1, u)

        @pl.when(u == 0)
        def _():
            start_forward(0, (2,), (0, 1, 2, 3))

        @pl.when(u == 2)
        def _():
            wait_partner(1)
            wait_first(1)
            start_forward(1, (1, 3), (0, 1, 2, 3))

        @pl.when(u == 4)
        def _():
            start_forward(1, (2,), (0, 1, 2, 3))

        w, d, j = step(u + 2)

        @pl.when((d > 0) & (u < 14))
        def _():
            for group in (0, 1):
                for e in (0, 1):
                    forward(group, w, d, 2 * j + e, True).wait_recv()

        @pl.when(u == 9)
        def _():
            for j in (0, 1):
                for group in (0, 1):
                    sum_first(group, 0, j)

        @pl.when(u == 14)
        def _():
            for group in (0, 1):
                sum_first(group, 1, 0)

    def body(v, _):
        u = 2 * v
        both(step(u + 1), step(u), 0)
        after(u)
        both(step(u + 2), step(u + 1), 1, u < 14)

        @pl.when(u < 14)
        def _():
            after(u + 1)

        return 0

    lax.fori_loop(0, 8, body, 0)
    both(None, step(15), 1)
    for group in (0, 1):
        sum_first(group, 1, 1)

    @pl.when(c == 0)
    def _():
        project(0)

    @pl.when(c == 1)
    def _():
        project(1)

    for copy in first:
        copy.wait_send()
    for w in (0, 1):
        for d in (1, 2, 3):
            for e in range(4):
                for group in (0, 1):
                    forward(group, w, d, e, False).wait_send()
    for group in (0, 1):
        for w in (0, 1):
            for j in (0, 1):
                for d in (1, 2, 3):
                    for copy in sends(group, w, d, j):
                        copy.wait_send()
            for i in (1, 2, 3):
                for copy in passes(group, w, i):
                    copy.wait_send()

            @pl.when(c != w)
            def _():
                for copy in passes(group, w, 0):
                    copy.wait_send()

    finish()


def shards(queries, keys, values, kv_len, causal_offset, out_weight):
    dma = pltpu.SemaphoreType.DMA
    hbm = pl.BlockSpec(memory_space=pl.ANY)
    smem = pl.BlockSpec(memory_space=pltpu.SMEM)

    def vmem(*shape, dtype=bf16):
        return pltpu.VMEM(shape, dtype)

    return pl.pallas_call(
        kernel,
        out_shape=jax.ShapeDtypeStruct((ROWS, COLS), f32),
        in_specs=[smem, smem, hbm, hbm, hbm, hbm],
        out_specs=pl.BlockSpec(memory_space=pltpu.VMEM),
        scratch_shapes=[
            vmem(ROWS * 8, HD),
            vmem(SLOTS * 4, HD),
            vmem(SLOTS * 4, HD),
            vmem(1024, 4608),
            vmem(BLOCK * 4, HD, dtype=f32),
            vmem(8, ROWS, HD),
            vmem(4, SLOTS, HD),
            vmem(4, SLOTS // HD, VROWS, HD),
            vmem(2, SLOTS, HD),
            vmem(2, SLOTS // HD, VROWS, HD),
            vmem(4, 4, 2, 4, ROWS, HD),
            vmem(2 * SLOTS, 256, dtype=f32),
            vmem(2 * SLOTS, 256, dtype=f32),
            vmem(2 * SLOTS, 256, dtype=f32),
            vmem(2 * SLOTS, 256, dtype=f32),
            vmem(2, 2, 8, 256, dtype=f32),
            vmem(2, 2, 4, 2, HD, 256),
            vmem(2, 2, 4, 2, 2, 256, dtype=f32),
            vmem(2, 2, 3, 2, HD, 256),
            vmem(2, 2, 3, 2, 2, 256, dtype=f32),
            vmem(2, 2, 4, HD, HD),
            vmem(2, 2, 4, 2, HD, dtype=f32),
            vmem(2, 2, 4, HD, HD),
            vmem(2, 2, 4, 2, HD, dtype=f32),
            vmem(ROWS, 1024),
            vmem(3, ROWS, COLS),
            vmem(ROWS, COLS, dtype=f32),
            vmem(3, ROWS, COLS),
            dma((2,)), dma((BLOCKS,)), dma((BLOCKS,)),
            dma, dma,
            dma((3, 2)), dma((3, 2)), dma((3, 2)), dma((3, 2)),
            dma((2, 2, 3, 4)), dma((2, 2, 3, 4)),
            dma((BLOCKS,)), dma((BLOCKS,)), dma((BLOCKS,)), dma((BLOCKS,)),
            dma((2, 2, 3, 2)), dma((2, 2, 3, 2)), dma((2, 2, 3, 2)), dma((2, 2, 3, 2)),
            dma((2, 2, 4)), dma((2, 2, 4)), dma((2, 2, 4)), dma((2, 2, 4)),
            dma((3,)), dma((3,)),
        ],
        compiler_params=pltpu.CompilerParams(
            collective_id=0, has_side_effects=True, vmem_limit_bytes=60 * 2**20
        ),
        name="attend",
    )(
        kv_len,
        causal_offset,
        queries.reshape(ROWS * 8, HD),
        keys.reshape(SLOTS * 4, HD),
        values.reshape(SLOTS * 4, HD),
        out_weight,
    )


def solution(mesh):
    placed = (
        P("seq", "head", None),
        P("seq", "head", None),
        P("seq", "head", None),
        P("seq"),
        P(),
        P("head", None),
    )
    return jax.shard_map(
        shards, mesh=mesh, in_specs=placed, out_specs=P("seq", "head"), check_vma=False
    )
```

```python
import math

import jax
import jax.numpy as jnp
from jax import lax
from jax.experimental import pallas as pl
from jax.experimental.pallas import tpu as pltpu
from jax.sharding import PartitionSpec as P

bf16 = jnp.bfloat16
f32 = jnp.float32
MESH = pl.DeviceIdType.MESH
score_scale = math.log2(math.e) / 12.0
masked_score = -1e30
HD = 128
ROWS = 64
SLOTS = 2048
VROWS = 144
COLS = 1152
BLOCK = 256
BLOCKS = SLOTS // BLOCK


def remote(src, dst, send_sem, recv_sem, device):
    return pltpu.make_async_remote_copy(
        src_ref=src,
        dst_ref=dst,
        send_sem=send_sem,
        recv_sem=recv_sem,
        device_id=device,
        device_id_type=MESH,
    )


def merge(parts):
    top = parts[0][1]
    for _, m, _ in parts[1:]:
        top = jnp.maximum(top, m)
    numer, denom = None, None
    for o, m, l in parts:
        factor = jnp.exp2(m - top)
        o = o.astype(f32) * factor
        l = l * factor
        numer = o if numer is None else numer + o
        denom = l if denom is None else denom + l
    return numer, top, denom


def kernel(
    len_ref, off_ref, q_hbm, k_hbm, v_hbm, w_hbm, out_ref,
    q_raw, k_raw, v_raw, w_vmem, wide, qs, ks, vs, kp, vp, qg, sa0, sa1, sb0, sb1, tops,
    o_own, m_own, in1, inm1, mid, midm, in2, inm2, lhs, part, total, inx,
    lsem, kl, vl, psend, precv, ysend, yrecv, zsend, zrecv, fsend, frecv,
    ksend, krecv, vsend, vrecv, s1s, s1r, s1ms, s1mr, s2s, s2r, s2ms, s2mr, xs, xr,
):
    seq = lax.axis_index("seq")
    head = lax.axis_index("head")
    z, y, c = seq // 8, (seq // 2) % 4, seq % 2
    p = 1 - c

    def dev(zt, yt, core):
        return ((zt * 4 + yt) * 2 + core, head)

    def ahead(index, d):
        return lax.rem(index + d, 4)

    partner = dev(z, y, p)

    load_q = pltpu.make_async_copy(q_hbm, q_raw, lsem.at[0])
    load_w = pltpu.make_async_copy(w_hbm, w_vmem, lsem.at[1])

    def load_kv(b):
        rows = pl.ds(pl.multiple_of(b * BLOCK * 4, BLOCK * 4), BLOCK * 4)
        return (
            pltpu.make_async_copy(k_hbm.at[rows], k_raw.at[rows], kl.at[b]),
            pltpu.make_async_copy(v_hbm.at[rows], v_raw.at[rows], vl.at[b]),
        )

    load_q.start()
    for b in range(BLOCKS):
        for copy in load_kv(b):
            copy.start()

    peers = [partner]
    for d in (1, 2, 3):
        for core in (0, 1):
            peers.append(dev(z, ahead(y, d), core))
            peers.append(dev(ahead(z, d), y, core))
        peers.append((seq, ahead(head, d)))
    barrier = pltpu.get_barrier_semaphore()
    for peer in peers:
        pl.semaphore_signal(barrier, inc=1, device_id=peer, device_id_type=MESH)

    load_q.wait()
    wide[0 : ROWS * 8, :] = q_raw[...].astype(f32)
    for h in range(8):
        qs[h] = wide[pl.ds(h, ROWS, stride=8), :].astype(bf16)
    qg[z, y, c] = qs[pl.ds(4 * c, 4)]

    length = len_ref[0]

    def prepare(b, _):
        for copy in load_kv(b):
            copy.wait()
        k0 = k_raw[0:8, :].astype(f32)
        rows = pl.ds(pl.multiple_of(b * BLOCK * 4, BLOCK * 4), BLOCK * 4)
        slots = pl.ds(pl.multiple_of(b * BLOCK, BLOCK), BLOCK)
        filled = lax.broadcasted_iota(jnp.int32, (BLOCK, HD), 0) + b * BLOCK < length
        wide[...] = k_raw[rows, :].astype(f32)
        for h in range(4):
            one = wide[pl.ds(h, BLOCK, stride=4), :]
            ks[h, slots, :] = jnp.where(filled, one, k0[h : h + 1, :]).astype(bf16)
        wide[...] = v_raw[rows, :].astype(f32)
        col = lax.broadcasted_iota(jnp.int32, (VROWS - HD, BLOCK), 1) + b * BLOCK
        row = lax.broadcasted_iota(jnp.int32, (VROWS - HD, BLOCK), 0)
        ones = jnp.where((col < length) & (row == 0), 1.0, 0.0).astype(bf16)
        for h in range(4):
            one = wide[pl.ds(h, BLOCK, stride=4), :]
            one = jnp.where(filled, one, 0.0).T.astype(bf16)
            for e in range(BLOCK // HD):
                lanes = slice(e * HD, (e + 1) * HD)
                vs[h, b * (BLOCK // HD) + e, 0:HD, :] = one[:, lanes]
                vs[h, b * (BLOCK // HD) + e, HD:VROWS, :] = ones[:, lanes]
        return 0

    def swap_kv(b):
        slots = pl.ds(pl.multiple_of(b * BLOCK, BLOCK), BLOCK)
        parts = pl.ds(b * (BLOCK // HD), BLOCK // HD)
        return (
            remote(ks.at[pl.ds(2 * p, 2), slots], kp.at[:, slots], ksend.at[b], krecv.at[b], partner),
            remote(
                vs.at[pl.ds(2 * p, 2), parts], vp.at[:, parts], vsend.at[b], vrecv.at[b], partner
            ),
        )

    pl.semaphore_wait(barrier, len(peers))

    first = [remote(qs.at[pl.ds(4 * p, 4)], qg.at[z, y, c], psend, precv, partner)]
    for d in (1, 3, 2):
        for core in (0, 1):
            first.append(
                remote(
                    qs.at[pl.ds(4 * core, 2)], qg.at[z, y, c, pl.ds(0, 2)],
                    ysend.at[d - 1, core], yrecv.at[d - 1, c], dev(z, ahead(y, d), core),
                )
            )
            first.append(
                remote(
                    qs.at[pl.ds(4 * core + 2, 2)], qg.at[z, y, c, pl.ds(2, 2)],
                    zsend.at[d - 1, core], zrecv.at[d - 1, c], dev(ahead(z, d), y, core),
                )
            )

    @pl.when(c == 0)
    def _():
        for copy in first:
            copy.start()

    def prepare_and_swap(b, _):
        prepare(b, 0)

        @pl.when(b > 0)
        def _():
            for copy in swap_kv(b - 1):
                copy.start()

        return 0

    lax.fori_loop(0, BLOCKS, prepare_and_swap, 0)

    @pl.when(c == 1)
    def _():
        for copy in first:
            copy.start()

    for copy in swap_kv(BLOCKS - 1):
        copy.start()
    load_w.start()

    last_chip = (z == 3) & (y == 3)
    offset = off_ref[0] - 30 * SLOTS

    def chips(group, d, j):
        if group == 0:
            return [(ahead(z, d), ahead(y, 2 * j + e)) for e in (0, 1)]
        return [(ahead(z, 2 * j + e), ahead(y, d)) for e in (0, 1)]

    def queries_of(group, w, d, j):
        parts = [qg[zq, yq, w, group * 2 + h] for zq, yq in chips(group, d, j) for h in (0, 1)]
        q = jnp.concatenate(parts, axis=0).astype(f32) * score_scale
        high = q.astype(bf16)
        low = (q - high.astype(f32)).astype(bf16)
        return jnp.concatenate([high, low], axis=1)

    def limit_of(group, w, d, j):
        lane = lax.broadcasted_iota(jnp.int32, (8, 256), 1)
        (za, ya), (zb, yb) = chips(group, d, j)
        chip = jnp.where(lane < HD, za * 4 + ya, zb * 4 + yb)
        row = chip * HD + w * ROWS + lane % ROWS
        return offset + row - lax.broadcasted_iota(jnp.int32, (8, 256), 0)

    def scores(qq, limit, group, shard, s_ref, m):
        k = ks[2 * c + group] if shard == 0 else kp[group]
        kk = jnp.concatenate([k, k], axis=1)
        s = lax.dot_general(kk, qq, (((1,), (1,)), ((), ())), preferred_element_type=f32)
        s = s.reshape(SLOTS // 8, 8, 256)
        if limit is not None:
            room = limit - SLOTS * (c if shard == 0 else p)
            s = jnp.stack(
                [jnp.where(room >= 8 * i, s[i], masked_score) for i in range(SLOTS // 8)]
            )
        s_ref[pl.ds(shard * SLOTS, SLOTS), :] = s.reshape(SLOTS, 256)
        return jnp.maximum(m, jnp.max(s, axis=0))

    def weigh(s_ref, m_now, group, shard, acc):
        s = s_ref[pl.ds(shard * SLOTS, SLOTS), :].reshape(SLOTS // 8, 8, 256)
        prob = jnp.exp2(s - m_now[None]).reshape(SLOTS, 256).astype(bf16)
        parts = [
            vs[2 * c + group, e] if shard == 0 else vp[group, e] for e in range(SLOTS // HD)
        ]
        return acc + jnp.dot(jnp.concatenate(parts, axis=1), prob, preferred_element_type=f32)

    score_refs = ((sa0, sa1), (sb0, sb1))

    def tiles(new, cur, side, causal):
        for group in (0, 1):
            m = jnp.full((8, 256), masked_score, f32)
            if new is not None:
                qq = queries_of(group, *new)
                limit = limit_of(group, *new) if causal else None
            if cur is not None:
                m_now = tops[side, group]
            acc = jnp.zeros((VROWS, 256), f32)
            for shard in (0, 1):
                if new is not None:
                    m = scores(qq, limit, group, shard, score_refs[1 - side][group], m)
                if cur is not None:
                    acc = weigh(score_refs[side][group], m_now, group, shard, acc)
            if cur is not None:
                w, d, j = cur
                o_own[group, w, d, j] = acc[:HD].astype(bf16)
                m_own[group, w, d, j, 0:1, :] = m_now[0:1]
                m_own[group, w, d, j, 1:2, :] = acc[HD : HD + 1]
            if new is not None:
                tops[1 - side, group] = jnp.broadcast_to(
                    jnp.max(m, axis=0, keepdims=True), (8, 256)
                )

    def both(new, cur, side, when=True):
        @pl.when(jnp.logical_not(last_chip) & when)
        def _():
            tiles(new, cur, side, False)

        @pl.when(last_chip & when)
        def _():
            tiles(new, cur, side, True)

    def step(u):
        w = u // 8
        k = lax.rem(u, 8) // 2
        k = lax.rem(k + w, 4)
        d = lax.rem(k * (k + 1) // 2, 4)
        return w, d, lax.rem(u, 2)

    def sends(group, w, d, j):
        target = dev(ahead(z, d), y, c) if group == 0 else dev(z, ahead(y, d), c)
        slot = (group, w, d - 1, j)
        return (
            remote(m_own.at[group, w, d, j], inm1.at[slot], s1ms.at[slot], s1mr.at[slot], target),
            remote(o_own.at[group, w, d, j], in1.at[slot], s1s.at[slot], s1r.at[slot], target),
        )

    def send_tile(group, u):
        w, d, j = step(u)

        @pl.when(d > 0)
        def _():
            for copy in sends(group, w, d, j):
                copy.start()

    def passes(group, w, i):
        if i == 0:
            target = partner
        else:
            target = dev(z, ahead(y, i), w) if group == 0 else dev(ahead(z, i), y, w)
        return (
            remote(
                midm.at[group, w, i], inm2.at[c, group, i],
                s2ms.at[group, w, i], s2mr.at[c, group, i], target,
            ),
            remote(
                mid.at[group, w, i], in2.at[c, group, i],
                s2s.at[group, w, i], s2r.at[c, group, i], target,
            ),
        )

    def sum_first(group, w, j):
        for d in (1, 2, 3):
            for copy in sends(group, w, d, j):
                copy.wait_recv()
        parts = [
            (o_own[group, w, 0, j], m_own[group, w, 0, j, 0:1, :], m_own[group, w, 0, j, 1:2, :])
        ]
        for d in range(3):
            parts.append(
                (in1[group, w, d, j], inm1[group, w, d, j, 0:1, :], inm1[group, w, d, j, 1:2, :])
            )
        numer, top, denom = merge(parts)
        for e in (0, 1):
            i = 2 * j + e
            lanes = slice(e * HD, (e + 1) * HD)
            mid[group, w, i] = numer[:, lanes].astype(bf16)
            midm[group, w, i, 0:1, :] = top[:, lanes]
            midm[group, w, i, 1:2, :] = denom[:, lanes]
        for e in (1, 0):
            i = 2 * j + e
            if i:
                for copy in passes(group, w, i):
                    copy.start()
            else:

                @pl.when(c != w)
                def _():
                    for copy in passes(group, w, 0):
                        copy.start()

                @pl.when(c == w)
                def _():
                    in2[c, group, 0] = mid[group, w, 0]
                    inm2[c, group, 0] = midm[group, w, 0]

    def exchange(d):
        return remote(
            part.at[d - 1], inx.at[d - 1], xs.at[d - 1], xr.at[d - 1], (seq, ahead(head, d))
        )

    def project(w):
        for group in (0, 1):
            for source in (0, 1):
                for i in range(4):
                    if i or source != w:
                        slot = (source, group, i)
                        remote(
                            midm.at[group, w, i], inm2.at[slot],
                            s2ms.at[group, w, i], s2mr.at[slot], partner,
                        ).wait_recv()
                        remote(
                            mid.at[group, w, i], in2.at[slot],
                            s2s.at[group, w, i], s2r.at[slot], partner,
                        ).wait_recv()
        for source in (0, 1):
            for group in (0, 1):
                parts = [
                    (
                        in2[source, group, i],
                        inm2[source, group, i, 0:1, :],
                        inm2[source, group, i, 1:2, :],
                    )
                    for i in range(4)
                ]
                numer, _, denom = merge(parts)
                rows = (numer / denom).T.astype(bf16)
                first_col = (source * 2 + group) * 2 * HD
                for h in (0, 1):
                    cols = slice(first_col + h * HD, first_col + (h + 1) * HD)
                    lhs[:, cols] = rows[h * ROWS : (h + 1) * ROWS]
        load_w.wait()
        left = lhs[...]
        for d in (2, 1, 3, 0):
            cols = pl.ds(pl.multiple_of(ahead(head, d) * COLS, HD), COLS)
            block = jnp.dot(left, w_vmem[:, cols], preferred_element_type=f32)
            if d:
                part[d - 1] = block.astype(bf16)
                exchange(d).start()
            else:
                total[...] = block

    def finish():
        for d in (1, 2, 3):
            exchange(d).wait()
        out_ref[...] = total[...] + (
            (inx[0].astype(f32) + inx[1].astype(f32)) + inx[2].astype(f32)
        )

    def wait_partner(core):
        @pl.when(c != core)
        def _():
            first[0].wait_recv()

    def wait_first(core):
        for d in (1, 2, 3):
            remote(
                qs.at[pl.ds(0, 2)], qg.at[z, ahead(y, 4 - d), core, pl.ds(0, 2)],
                ysend.at[d - 1, core], yrecv.at[d - 1, core], partner,
            ).wait_recv()
            remote(
                qs.at[pl.ds(0, 2)], qg.at[ahead(z, 4 - d), y, core, pl.ds(2, 2)],
                zsend.at[d - 1, core], zrecv.at[d - 1, core], partner,
            ).wait_recv()

    def forward(group, w, d, e, back):
        if group == 0:
            src = qg.at[ahead(z, d) if back else z, ahead(y, e), w, pl.ds(0, 2)]
            target = dev(ahead(z, 4 - d), y, c)
        else:
            src = qg.at[ahead(z, e), ahead(y, d) if back else y, w, pl.ds(2, 2)]
            target = dev(z, ahead(y, 4 - d), c)
        slot = (group, w, d - 1, e)
        return remote(src, src, fsend.at[slot], frecv.at[slot], target)

    def start_forward(w, ds, es):
        for e in es:
            for d in ds:
                for group in (0, 1):
                    forward(group, w, d, e, False).start()

    wait_partner(0)
    start_forward(0, (1, 3), (0,))
    wait_first(0)
    start_forward(0, (1, 3), (1, 2, 3))

    def wait_swap(b, _):
        for copy in swap_kv(b):
            copy.wait()
        return 0

    def open_with(shard, causal):
        for group in (0, 1):
            qq = queries_of(group, *step(0))
            limit = limit_of(group, *step(0)) if causal else None
            m = tops[0, group] if shard else jnp.full((8, 256), masked_score, f32)
            m = scores(qq, limit, group, shard, score_refs[0][group], m)
            tops[0, group] = jnp.broadcast_to(jnp.max(m, axis=0, keepdims=True), (8, 256))

    for shard in (0, 1):
        if shard:
            lax.fori_loop(0, BLOCKS, wait_swap, 0)

        @pl.when(jnp.logical_not(last_chip))
        def _():
            open_with(shard, False)

        @pl.when(last_chip)
        def _():
            open_with(shard, True)

    def after(u):
        send_tile(0, u)
        send_tile(1, u)

        @pl.when(u == 0)
        def _():
            start_forward(0, (2,), (0, 1, 2, 3))

        @pl.when(u == 2)
        def _():
            wait_partner(1)
            wait_first(1)
            start_forward(1, (1, 3), (0, 1, 2, 3))

        @pl.when(u == 4)
        def _():
            start_forward(1, (2,), (0, 1, 2, 3))

        w, d, j = step(u + 2)

        @pl.when((d > 0) & (u < 14))
        def _():
            for group in (0, 1):
                for e in (0, 1):
                    forward(group, w, d, 2 * j + e, True).wait_recv()

        @pl.when(u == 9)
        def _():
            for j in (0, 1):
                for group in (0, 1):
                    sum_first(group, 0, j)

        @pl.when(u == 14)
        def _():
            for group in (0, 1):
                sum_first(group, 1, 0)

    def body(v, _):
        u = 2 * v
        both(step(u + 1), step(u), 0)
        after(u)
        both(step(u + 2), step(u + 1), 1, u < 14)

        @pl.when(u < 14)
        def _():
            after(u + 1)

        return 0

    lax.fori_loop(0, 8, body, 0)
    both(None, step(15), 1)
    for group in (0, 1):
        sum_first(group, 1, 1)

    @pl.when(c == 0)
    def _():
        project(0)

    @pl.when(c == 1)
    def _():
        project(1)

    for copy in first:
        copy.wait_send()
    for w in (0, 1):
        for d in (1, 2, 3):
            for e in range(4):
                for group in (0, 1):
                    forward(group, w, d, e, False).wait_send()
    for group in (0, 1):
        for w in (0, 1):
            for j in (0, 1):
                for d in (1, 2, 3):
                    for copy in sends(group, w, d, j):
                        copy.wait_send()
            for i in (1, 2, 3):
                for copy in passes(group, w, i):
                    copy.wait_send()

            @pl.when(c != w)
            def _():
                for copy in passes(group, w, 0):
                    copy.wait_send()

    finish()


def shards(queries, keys, values, kv_len, causal_offset, out_weight):
    dma = pltpu.SemaphoreType.DMA
    hbm = pl.BlockSpec(memory_space=pltpu.HBM)
    smem = pl.BlockSpec(memory_space=pltpu.SMEM)

    def vmem(*shape, dtype=bf16):
        return pltpu.VMEM(shape, dtype)

    return pl.pallas_call(
        kernel,
        out_shape=jax.ShapeDtypeStruct((ROWS, COLS), f32),
        in_specs=[smem, smem, hbm, hbm, hbm, hbm],
        out_specs=pl.BlockSpec(memory_space=pltpu.VMEM),
        scratch_shapes=[
            vmem(ROWS * 8, HD),
            vmem(SLOTS * 4, HD),
            vmem(SLOTS * 4, HD),
            vmem(1024, 4608),
            vmem(BLOCK * 4, HD, dtype=f32),
            vmem(8, ROWS, HD),
            vmem(4, SLOTS, HD),
            vmem(4, SLOTS // HD, VROWS, HD),
            vmem(2, SLOTS, HD),
            vmem(2, SLOTS // HD, VROWS, HD),
            vmem(4, 4, 2, 4, ROWS, HD),
            vmem(2 * SLOTS, 256, dtype=f32),
            vmem(2 * SLOTS, 256, dtype=f32),
            vmem(2 * SLOTS, 256, dtype=f32),
            vmem(2 * SLOTS, 256, dtype=f32),
            vmem(2, 2, 8, 256, dtype=f32),
            vmem(2, 2, 4, 2, HD, 256),
            vmem(2, 2, 4, 2, 2, 256, dtype=f32),
            vmem(2, 2, 3, 2, HD, 256),
            vmem(2, 2, 3, 2, 2, 256, dtype=f32),
            vmem(2, 2, 4, HD, HD),
            vmem(2, 2, 4, 2, HD, dtype=f32),
            vmem(2, 2, 4, HD, HD),
            vmem(2, 2, 4, 2, HD, dtype=f32),
            vmem(ROWS, 1024),
            vmem(3, ROWS, COLS),
            vmem(ROWS, COLS, dtype=f32),
            vmem(3, ROWS, COLS),
            dma((2,)), dma((BLOCKS,)), dma((BLOCKS,)),
            dma, dma,
            dma((3, 2)), dma((3, 2)), dma((3, 2)), dma((3, 2)),
            dma((2, 2, 3, 4)), dma((2, 2, 3, 4)),
            dma((BLOCKS,)), dma((BLOCKS,)), dma((BLOCKS,)), dma((BLOCKS,)),
            dma((2, 2, 3, 2)), dma((2, 2, 3, 2)), dma((2, 2, 3, 2)), dma((2, 2, 3, 2)),
            dma((2, 2, 4)), dma((2, 2, 4)), dma((2, 2, 4)), dma((2, 2, 4)),
            dma((3,)), dma((3,)),
        ],
        compiler_params=pltpu.CompilerParams(
            collective_id=0, has_side_effects=True, vmem_limit_bytes=53 * 2**20
        ),
        name="attend",
    )(
        kv_len,
        causal_offset,
        queries.reshape(ROWS * 8, HD),
        keys.reshape(SLOTS * 4, HD),
        values.reshape(SLOTS * 4, HD),
        out_weight,
    )


def solution(mesh):
    placed = (
        P("seq", "head", None),
        P("seq", "head", None),
        P("seq", "head", None),
        P("seq"),
        P(),
        P("head", None),
    )
    return jax.shard_map(
        shards, mesh=mesh, in_specs=placed, out_specs=P("seq", "head"), check_vma=False
    )
```

```python
import math

import jax
import jax.numpy as jnp
from jax import lax
from jax.experimental import pallas as pl
from jax.experimental.pallas import tpu as pltpu
from jax.sharding import PartitionSpec as P

bf16 = jnp.bfloat16
f32 = jnp.float32
MESH = pl.DeviceIdType.MESH
score_scale = math.log2(math.e) / 12.0
masked_score = -1e30
HD = 128
ROWS = 64
SLOTS = 2048
VROWS = 144
COLS = 1152
BLOCK = 256
BLOCKS = SLOTS // BLOCK


def remote(src, dst, send_sem, recv_sem, device):
    return pltpu.make_async_remote_copy(
        src_ref=src,
        dst_ref=dst,
        send_sem=send_sem,
        recv_sem=recv_sem,
        device_id=device,
        device_id_type=MESH,
    )


def merge(parts):
    top = parts[0][1]
    for _, m, _ in parts[1:]:
        top = jnp.maximum(top, m)
    numer, denom = None, None
    for o, m, l in parts:
        factor = jnp.exp2(m - top)
        o = o.astype(f32) * factor
        l = l * factor
        numer = o if numer is None else numer + o
        denom = l if denom is None else denom + l
    return numer, top, denom


def kernel(
    len_ref, off_ref, q_hbm, k_hbm, v_hbm, w_hbm, out_ref,
    q_raw, k_raw, v_raw, w_vmem, wide, qs, ks, vs, kp, vp, qg, sa0, sa1, sb0, sb1, tops,
    o_own, m_own, in1, inm1, mid, midm, in2, inm2, lhs, part, total, inx,
    lsem, kl, vl, psend, precv, ysend, yrecv, zsend, zrecv, fsend, frecv,
    ksend, krecv, vsend, vrecv, s1s, s1r, s1ms, s1mr, s2s, s2r, s2ms, s2mr, xs, xr,
):
    seq = lax.axis_index("seq")
    head = lax.axis_index("head")
    z, y, c = seq // 8, (seq // 2) % 4, seq % 2
    p = 1 - c

    def dev(zt, yt, core):
        return ((zt * 4 + yt) * 2 + core, head)

    def ahead(index, d):
        return lax.rem(index + d, 4)

    partner = dev(z, y, p)

    load_q = pltpu.make_async_copy(q_hbm, q_raw, lsem.at[0])
    load_w = pltpu.make_async_copy(w_hbm, w_vmem, lsem.at[1])

    def load_kv(b):
        rows = pl.ds(pl.multiple_of(b * BLOCK * 4, BLOCK * 4), BLOCK * 4)
        return (
            pltpu.make_async_copy(k_hbm.at[rows], k_raw.at[rows], kl.at[b]),
            pltpu.make_async_copy(v_hbm.at[rows], v_raw.at[rows], vl.at[b]),
        )

    load_q.start()
    for b in range(BLOCKS):
        for copy in load_kv(b):
            copy.start()

    peers = [partner]
    for d in (1, 2, 3):
        for core in (0, 1):
            peers.append(dev(z, ahead(y, d), core))
            peers.append(dev(ahead(z, d), y, core))
        peers.append((seq, ahead(head, d)))
    barrier = pltpu.get_barrier_semaphore()
    for peer in peers:
        pl.semaphore_signal(barrier, inc=1, device_id=peer, device_id_type=MESH)

    load_q.wait()
    wide[0 : ROWS * 8, :] = q_raw[...].astype(f32)
    for h in range(8):
        qs[h] = wide[pl.ds(h, ROWS, stride=8), :].astype(bf16)
    qg[z, y, c] = qs[pl.ds(4 * c, 4)]

    length = len_ref[0]

    def prepare(b, _):
        for copy in load_kv(b):
            copy.wait()
        k0 = k_raw[0:8, :].astype(f32)
        rows = pl.ds(pl.multiple_of(b * BLOCK * 4, BLOCK * 4), BLOCK * 4)
        slots = pl.ds(pl.multiple_of(b * BLOCK, BLOCK), BLOCK)
        filled = lax.broadcasted_iota(jnp.int32, (BLOCK, HD), 0) + b * BLOCK < length
        wide[...] = k_raw[rows, :].astype(f32)
        for h in range(4):
            one = wide[pl.ds(h, BLOCK, stride=4), :]
            ks[h, slots, :] = jnp.where(filled, one, k0[h : h + 1, :]).astype(bf16)
        wide[...] = v_raw[rows, :].astype(f32)
        col = lax.broadcasted_iota(jnp.int32, (VROWS - HD, BLOCK), 1) + b * BLOCK
        row = lax.broadcasted_iota(jnp.int32, (VROWS - HD, BLOCK), 0)
        ones = jnp.where((col < length) & (row == 0), 1.0, 0.0).astype(bf16)
        for h in range(4):
            one = wide[pl.ds(h, BLOCK, stride=4), :]
            one = jnp.where(filled, one, 0.0).T.astype(bf16)
            for e in range(BLOCK // HD):
                lanes = slice(e * HD, (e + 1) * HD)
                vs[h, b * (BLOCK // HD) + e, 0:HD, :] = one[:, lanes]
                vs[h, b * (BLOCK // HD) + e, HD:VROWS, :] = ones[:, lanes]
        return 0

    def swap_kv(b):
        slots = pl.ds(pl.multiple_of(b * BLOCK, BLOCK), BLOCK)
        parts = pl.ds(b * (BLOCK // HD), BLOCK // HD)
        return (
            remote(ks.at[pl.ds(2 * p, 2), slots], kp.at[:, slots], ksend.at[b], krecv.at[b], partner),
            remote(
                vs.at[pl.ds(2 * p, 2), parts], vp.at[:, parts], vsend.at[b], vrecv.at[b], partner
            ),
        )

    pl.semaphore_wait(barrier, len(peers))

    first = [remote(qs.at[pl.ds(4 * p, 4)], qg.at[z, y, c], psend, precv, partner)]
    for d in (1, 3, 2):
        for core in (0, 1):
            first.append(
                remote(
                    qs.at[pl.ds(4 * core, 2)], qg.at[z, y, c, pl.ds(0, 2)],
                    ysend.at[d - 1, core], yrecv.at[d - 1, c], dev(z, ahead(y, d), core),
                )
            )
            first.append(
                remote(
                    qs.at[pl.ds(4 * core + 2, 2)], qg.at[z, y, c, pl.ds(2, 2)],
                    zsend.at[d - 1, core], zrecv.at[d - 1, c], dev(ahead(z, d), y, core),
                )
            )

    @pl.when(c == 0)
    def _():
        for copy in first:
            copy.start()

    def prepare_and_swap(b, _):
        prepare(b, 0)

        @pl.when(b > 0)
        def _():
            for copy in swap_kv(b - 1):
                copy.start()

        return 0

    lax.fori_loop(0, BLOCKS, prepare_and_swap, 0)

    @pl.when(c == 1)
    def _():
        for copy in first:
            copy.start()

    for copy in swap_kv(BLOCKS - 1):
        copy.start()
    load_w.start()

    last_chip = (z == 3) & (y == 3)
    offset = off_ref[0] - 30 * SLOTS

    def chips(group, d, j):
        if group == 0:
            return [(ahead(z, d), ahead(y, 2 * j + e)) for e in (0, 1)]
        return [(ahead(z, 2 * j + e), ahead(y, d)) for e in (0, 1)]

    def queries_of(group, w, d, j):
        parts = [qg[zq, yq, w, group * 2 + h] for zq, yq in chips(group, d, j) for h in (0, 1)]
        q = jnp.concatenate(parts, axis=0).astype(f32) * score_scale
        high = q.astype(bf16)
        low = (q - high.astype(f32)).astype(bf16)
        return jnp.concatenate([high, low], axis=1)

    def limit_of(group, w, d, j):
        lane = lax.broadcasted_iota(jnp.int32, (8, 256), 1)
        (za, ya), (zb, yb) = chips(group, d, j)
        chip = jnp.where(lane < HD, za * 4 + ya, zb * 4 + yb)
        row = chip * HD + w * ROWS + lane % ROWS
        return offset + row - lax.broadcasted_iota(jnp.int32, (8, 256), 0)

    def scores(qq, limit, group, shard, s_ref, m):
        k = ks[2 * c + group] if shard == 0 else kp[group]
        kk = jnp.concatenate([k, k], axis=1)
        s = lax.dot_general(kk, qq, (((1,), (1,)), ((), ())), preferred_element_type=f32)
        s = s.reshape(SLOTS // 8, 8, 256)
        if limit is not None:
            room = limit - SLOTS * (c if shard == 0 else p)
            s = jnp.stack(
                [jnp.where(room >= 8 * i, s[i], masked_score) for i in range(SLOTS // 8)]
            )
        s_ref[pl.ds(shard * SLOTS, SLOTS), :] = s.reshape(SLOTS, 256)
        return jnp.maximum(m, jnp.max(s, axis=0))

    def weigh(s_ref, m_now, group, shard, acc):
        s = s_ref[pl.ds(shard * SLOTS, SLOTS), :].reshape(SLOTS // 8, 8, 256)
        prob = jnp.exp2(s - m_now[None]).reshape(SLOTS, 256).astype(bf16)
        parts = [
            vs[2 * c + group, e] if shard == 0 else vp[group, e] for e in range(SLOTS // HD)
        ]
        return acc + jnp.dot(jnp.concatenate(parts, axis=1), prob, preferred_element_type=f32)

    score_refs = ((sa0, sa1), (sb0, sb1))

    def tiles(new, cur, side, causal):
        for group in (0, 1):
            m = jnp.full((8, 256), masked_score, f32)
            if new is not None:
                qq = queries_of(group, *new)
                limit = limit_of(group, *new) if causal else None
            if cur is not None:
                m_now = tops[side, group]
            acc = jnp.zeros((VROWS, 256), f32)
            for shard in (0, 1):
                if new is not None:
                    m = scores(qq, limit, group, shard, score_refs[1 - side][group], m)
                if cur is not None:
                    acc = weigh(score_refs[side][group], m_now, group, shard, acc)
            if cur is not None:
                w, d, j = cur
                o_own[group, w, d, j] = acc[:HD].astype(bf16)
                m_own[group, w, d, j, 0:1, :] = m_now[0:1]
                m_own[group, w, d, j, 1:2, :] = acc[HD : HD + 1]
            if new is not None:
                tops[1 - side, group] = jnp.broadcast_to(
                    jnp.max(m, axis=0, keepdims=True), (8, 256)
                )

    def both(new, cur, side, when=True):
        @pl.when(jnp.logical_not(last_chip) & when)
        def _():
            tiles(new, cur, side, False)

        @pl.when(last_chip & when)
        def _():
            tiles(new, cur, side, True)

    def step(u):
        w = u // 8
        k = lax.rem(u, 8) // 2
        k = lax.rem(k + w, 4)
        d = lax.rem(k * (k + 1) // 2, 4)
        return w, d, lax.rem(u, 2)

    def sends(group, w, d, j):
        target = dev(ahead(z, d), y, c) if group == 0 else dev(z, ahead(y, d), c)
        slot = (group, w, d - 1, j)
        return (
            remote(m_own.at[group, w, d, j], inm1.at[slot], s1ms.at[slot], s1mr.at[slot], target),
            remote(o_own.at[group, w, d, j], in1.at[slot], s1s.at[slot], s1r.at[slot], target),
        )

    def send_tile(group, u):
        w, d, j = step(u)

        @pl.when(d > 0)
        def _():
            for copy in sends(group, w, d, j):
                copy.start()

    def passes(group, w, i):
        if i == 0:
            target = partner
        else:
            target = dev(z, ahead(y, i), w) if group == 0 else dev(ahead(z, i), y, w)
        return (
            remote(
                midm.at[group, w, i], inm2.at[c, group, i],
                s2ms.at[group, w, i], s2mr.at[c, group, i], target,
            ),
            remote(
                mid.at[group, w, i], in2.at[c, group, i],
                s2s.at[group, w, i], s2r.at[c, group, i], target,
            ),
        )

    def sum_first(group, w, j):
        for d in (1, 2, 3):
            for copy in sends(group, w, d, j):
                copy.wait_recv()
        parts = [
            (o_own[group, w, 0, j], m_own[group, w, 0, j, 0:1, :], m_own[group, w, 0, j, 1:2, :])
        ]
        for d in range(3):
            parts.append(
                (in1[group, w, d, j], inm1[group, w, d, j, 0:1, :], inm1[group, w, d, j, 1:2, :])
            )
        numer, top, denom = merge(parts)
        for e in (0, 1):
            i = 2 * j + e
            lanes = slice(e * HD, (e + 1) * HD)
            mid[group, w, i] = numer[:, lanes].astype(bf16)
            midm[group, w, i, 0:1, :] = top[:, lanes]
            midm[group, w, i, 1:2, :] = denom[:, lanes]
        for e in (1, 0):
            i = 2 * j + e
            if i:
                for copy in passes(group, w, i):
                    copy.start()
            else:

                @pl.when(c != w)
                def _():
                    for copy in passes(group, w, 0):
                        copy.start()

                @pl.when(c == w)
                def _():
                    in2[c, group, 0] = mid[group, w, 0]
                    inm2[c, group, 0] = midm[group, w, 0]

    def exchange(d):
        return remote(
            part.at[d - 1], inx.at[d - 1], xs.at[d - 1], xr.at[d - 1], (seq, ahead(head, d))
        )

    def project(w):
        for group in (0, 1):
            for source in (0, 1):
                for i in range(4):
                    if i or source != w:
                        slot = (source, group, i)
                        remote(
                            midm.at[group, w, i], inm2.at[slot],
                            s2ms.at[group, w, i], s2mr.at[slot], partner,
                        ).wait_recv()
                        remote(
                            mid.at[group, w, i], in2.at[slot],
                            s2s.at[group, w, i], s2r.at[slot], partner,
                        ).wait_recv()
        for source in (0, 1):
            for group in (0, 1):
                parts = [
                    (
                        in2[source, group, i],
                        inm2[source, group, i, 0:1, :],
                        inm2[source, group, i, 1:2, :],
                    )
                    for i in range(4)
                ]
                numer, _, denom = merge(parts)
                rows = (numer / denom).T.astype(bf16)
                first_col = (source * 2 + group) * 2 * HD
                for h in (0, 1):
                    cols = slice(first_col + h * HD, first_col + (h + 1) * HD)
                    lhs[:, cols] = rows[h * ROWS : (h + 1) * ROWS]
        load_w.wait()
        left = lhs[...]
        for d in (2, 1, 3, 0):
            cols = pl.ds(pl.multiple_of(ahead(head, d) * COLS, HD), COLS)
            block = jnp.dot(left, w_vmem[:, cols], preferred_element_type=f32)
            if d:
                part[d - 1] = block.astype(bf16)
                exchange(d).start()
            else:
                total[...] = block

    def finish():
        for d in (1, 2, 3):
            exchange(d).wait()
        out_ref[...] = total[...] + (
            (inx[0].astype(f32) + inx[1].astype(f32)) + inx[2].astype(f32)
        )

    def wait_partner(core):
        @pl.when(c != core)
        def _():
            first[0].wait_recv()

    def wait_first(core):
        for d in (1, 2, 3):
            remote(
                qs.at[pl.ds(0, 2)], qg.at[z, ahead(y, 4 - d), core, pl.ds(0, 2)],
                ysend.at[d - 1, core], yrecv.at[d - 1, core], partner,
            ).wait_recv()
            remote(
                qs.at[pl.ds(0, 2)], qg.at[ahead(z, 4 - d), y, core, pl.ds(2, 2)],
                zsend.at[d - 1, core], zrecv.at[d - 1, core], partner,
            ).wait_recv()

    def forward(group, w, d, e, back):
        if group == 0:
            src = qg.at[ahead(z, d) if back else z, ahead(y, e), w, pl.ds(0, 2)]
            target = dev(ahead(z, 4 - d), y, c)
        else:
            src = qg.at[ahead(z, e), ahead(y, d) if back else y, w, pl.ds(2, 2)]
            target = dev(z, ahead(y, 4 - d), c)
        slot = (group, w, d - 1, e)
        return remote(src, src, fsend.at[slot], frecv.at[slot], target)

    def start_forward(w, ds, es):
        for e in es:
            for d in ds:
                for group in (0, 1):
                    forward(group, w, d, e, False).start()

    wait_partner(0)
    start_forward(0, (1, 3), (0,))
    wait_first(0)
    start_forward(0, (1, 3), (1, 2, 3))

    def wait_swap(b, _):
        for copy in swap_kv(b):
            copy.wait()
        return 0

    def open_with(shard, causal):
        for group in (0, 1):
            qq = queries_of(group, *step(0))
            limit = limit_of(group, *step(0)) if causal else None
            m = tops[0, group] if shard else jnp.full((8, 256), masked_score, f32)
            m = scores(qq, limit, group, shard, score_refs[0][group], m)
            tops[0, group] = jnp.broadcast_to(jnp.max(m, axis=0, keepdims=True), (8, 256))

    for shard in (0, 1):
        if shard:
            lax.fori_loop(0, BLOCKS, wait_swap, 0)

        @pl.when(jnp.logical_not(last_chip))
        def _():
            open_with(shard, False)

        @pl.when(last_chip)
        def _():
            open_with(shard, True)

    def after(u):
        send_tile(0, u)
        send_tile(1, u)

        @pl.when(u == 0)
        def _():
            start_forward(0, (2,), (0, 1, 2, 3))

        @pl.when(u == 1)
        def _():
            wait_partner(1)
            wait_first(1)
            start_forward(1, (1, 3), (0, 1, 2, 3))

        @pl.when(u == 3)
        def _():
            start_forward(1, (2,), (0, 1, 2, 3))

        w, d, j = step(u + 2)

        @pl.when((d > 0) & (u < 14))
        def _():
            for group in (0, 1):
                for e in (0, 1):
                    forward(group, w, d, 2 * j + e, True).wait_recv()

        @pl.when(u == 11)
        def _():
            for j in (0, 1):
                for group in (0, 1):
                    sum_first(group, 0, j)

        @pl.when(u == 14)
        def _():
            for group in (0, 1):
                sum_first(group, 1, 0)

    def body(v, _):
        u = 2 * v
        both(step(u + 1), step(u), 0)
        after(u)
        both(step(u + 2), step(u + 1), 1, u < 14)

        @pl.when(u < 14)
        def _():
            after(u + 1)

        return 0

    lax.fori_loop(0, 8, body, 0)
    both(None, step(15), 1)
    for group in (0, 1):
        sum_first(group, 1, 1)

    @pl.when(c == 0)
    def _():
        project(0)

    @pl.when(c == 1)
    def _():
        project(1)

    for copy in first:
        copy.wait_send()
    for w in (0, 1):
        for d in (1, 2, 3):
            for e in range(4):
                for group in (0, 1):
                    forward(group, w, d, e, False).wait_send()
    for group in (0, 1):
        for w in (0, 1):
            for j in (0, 1):
                for d in (1, 2, 3):
                    for copy in sends(group, w, d, j):
                        copy.wait_send()
            for i in (1, 2, 3):
                for copy in passes(group, w, i):
                    copy.wait_send()

            @pl.when(c != w)
            def _():
                for copy in passes(group, w, 0):
                    copy.wait_send()

    finish()


def shards(queries, keys, values, kv_len, causal_offset, out_weight):
    dma = pltpu.SemaphoreType.DMA
    hbm = pl.BlockSpec(memory_space=pltpu.HBM)
    smem = pl.BlockSpec(memory_space=pltpu.SMEM)

    def vmem(*shape, dtype=bf16):
        return pltpu.VMEM(shape, dtype)

    return pl.pallas_call(
        kernel,
        out_shape=jax.ShapeDtypeStruct((ROWS, COLS), f32),
        in_specs=[smem, smem, hbm, hbm, hbm, hbm],
        out_specs=pl.BlockSpec(memory_space=pltpu.VMEM),
        scratch_shapes=[
            vmem(ROWS * 8, HD),
            vmem(SLOTS * 4, HD),
            vmem(SLOTS * 4, HD),
            vmem(1024, 4608),
            vmem(BLOCK * 4, HD, dtype=f32),
            vmem(8, ROWS, HD),
            vmem(4, SLOTS, HD),
            vmem(4, SLOTS // HD, VROWS, HD),
            vmem(2, SLOTS, HD),
            vmem(2, SLOTS // HD, VROWS, HD),
            vmem(4, 4, 2, 4, ROWS, HD),
            vmem(2 * SLOTS, 256, dtype=f32),
            vmem(2 * SLOTS, 256, dtype=f32),
            vmem(2 * SLOTS, 256, dtype=f32),
            vmem(2 * SLOTS, 256, dtype=f32),
            vmem(2, 2, 8, 256, dtype=f32),
            vmem(2, 2, 4, 2, HD, 256),
            vmem(2, 2, 4, 2, 2, 256, dtype=f32),
            vmem(2, 2, 3, 2, HD, 256),
            vmem(2, 2, 3, 2, 2, 256, dtype=f32),
            vmem(2, 2, 4, HD, HD),
            vmem(2, 2, 4, 2, HD, dtype=f32),
            vmem(2, 2, 4, HD, HD),
            vmem(2, 2, 4, 2, HD, dtype=f32),
            vmem(ROWS, 1024),
            vmem(3, ROWS, COLS),
            vmem(ROWS, COLS, dtype=f32),
            vmem(3, ROWS, COLS),
            dma((2,)), dma((BLOCKS,)), dma((BLOCKS,)),
            dma, dma,
            dma((3, 2)), dma((3, 2)), dma((3, 2)), dma((3, 2)),
            dma((2, 2, 3, 4)), dma((2, 2, 3, 4)),
            dma((BLOCKS,)), dma((BLOCKS,)), dma((BLOCKS,)), dma((BLOCKS,)),
            dma((2, 2, 3, 2)), dma((2, 2, 3, 2)), dma((2, 2, 3, 2)), dma((2, 2, 3, 2)),
            dma((2, 2, 4)), dma((2, 2, 4)), dma((2, 2, 4)), dma((2, 2, 4)),
            dma((3,)), dma((3,)),
        ],
        compiler_params=pltpu.CompilerParams(
            collective_id=0, has_side_effects=True, vmem_limit_bytes=53 * 2**20
        ),
        name="attend",
    )(
        kv_len,
        causal_offset,
        queries.reshape(ROWS * 8, HD),
        keys.reshape(SLOTS * 4, HD),
        values.reshape(SLOTS * 4, HD),
        out_weight,
    )


def solution(mesh):
    placed = (
        P("seq", "head", None),
        P("seq", "head", None),
        P("seq", "head", None),
        P("seq"),
        P(),
        P("head", None),
    )
    return jax.shard_map(
        shards, mesh=mesh, in_specs=placed, out_specs=P("seq", "head"), check_vma=False
    )
```
